256 devices in a mesh: wave: 32 (over x, z_hi, core), level: 8 (over y, z_lo).
Axes of the slice: x: 4, y: 4, z: 8 (z_hi: 4, z_lo: 2; z = z_hi * 2 + z_lo), core: 2. Of those that a mesh axis runs over, the one named last changes fastest.
Arguments:
- state: float32 [4, 64, 256, 2, 256], P(None, 'level', 'wave'), may hold values from -0.02 to 0.02
- legendre: float32 [256, 384, 256], P('wave'), may hold values from -6 to 6
- lat_weight: float32 [384], P('wave'), may hold values from 0.8 to 2
- modes: float32 [64, 64], replicated, may hold values from -1 to 1, as said below
- mode_rates: float32 [64], replicated, may hold values from 1e-05 to 0.003
- diffusion: float32 [4], replicated, may hold values from 0.3 to 3
- norm_gain: float32 [256], replicated, may hold values from 0.5 to 1.5
- w_first: bfloat16 [1024, 256], replicated, may hold values from -0.375 to 0.375
- b_first: float32 [1024], replicated, may hold values from -3 to 3
- w_second: bfloat16 [1024, 1024], replicated, may hold values from -0.1875 to 0.1875
- b_second: float32 [1024], replicated, may hold values from -3 to 3
- w_third: bfloat16 [256, 1024], replicated, may hold values from -0.1875 to 0.1875
- b_third: float32 [256], replicated, may hold values from -1.2 to 1.2
Outputs:
- next_state: float32 [4, 64, 256, 2, 256], P(None, 'level', 'wave')
The draws below stay inside these ranges and needn't reach their ends.
Inputs may be any that keep to these rules, and one draw needn't show every extreme that they name: `modes`: orthogonal: its transpose is its inverse.
All inputs are finite; a program needn't handle non-finite values.
Results may differ from the reference program's by a relative error of at most 0.0011.
Values may be sent and summed in bfloat16 or wider, within the bound.
A program may use at most 128 MiB of HBM per device.

```python
import math
import jax
import jax.numpy as jnp
from jax import lax

F = 4
LEV = 64
M = 256
LAT = 384
LON = 768
HID = 1024


def draw_modes(key, part):
    random_matrix = jax.random.normal(key, (LEV, LEV), jnp.float32)
    factors = jnp.linalg.qr(random_matrix)
    return factors[0].astype(jnp.float32)


def level_of(rng, extent, shards, least, largest):
    level, own = 1.0, jax.random.fold_in(rng, 6)
    for axis_at, shards_of in shards:
        heights = jnp.exp(jax.random.uniform(jax.random.fold_in(own, axis_at), (shards_of,), jnp.float32, least / len(shards), largest / len(shards)))
        level = level * jnp.repeat(heights, extent[axis_at] // shards_of).reshape([-1 if axis == axis_at else 1 for axis in range(len(extent))])
    return level


def gaussian(key, dims, deviation, bound, shards=(), kind=jnp.bfloat16):
    values = deviation * jax.random.normal(key, dims, jnp.float32)
    if shards:
        values = values * level_of(key, dims, shards, -0.22, 0.18)
    return jnp.clip(values, -bound, bound).astype(kind)


def setup_inputs(seed: int = 0) -> dict:
    key_of = jax.random.split(jax.random.key(seed), 14)
    state = gaussian(key_of[0], (F, LEV, M, 2, M), 0.003, 0.02, ((1, 8), (2, 32)), jnp.float32)
    legendre = gaussian(key_of[1], (M, LAT, M), 1.0, 6.0, ((0, 32),), jnp.float32)
    lat_weight = jnp.clip(0.8 + 1.2 * jax.random.uniform(key_of[2], (LAT,), jnp.float32) ** level_of(key_of[2], (LAT,), ((0, 32),), -0.2, 0.2), 0.8, 2.0)
    modes = draw_modes(jax.random.fold_in(key_of[13], 71), 0)
    mode_rates = jnp.clip(jnp.exp(jax.random.uniform(key_of[4], (LEV,), jnp.float32, math.log(9.999999747378752e-06), math.log(0.003))), 9.999999747378752e-06, 0.003)
    diffusion = jnp.clip(jnp.exp(jax.random.uniform(key_of[5], (F,), jnp.float32, math.log(0.3), math.log(3.0))), 0.3, 3.0)
    norm_gain = jnp.clip(1.0 + 0.1 * jax.random.normal(key_of[6], (F * LEV,), jnp.float32), 0.5, 1.5)
    w_first = gaussian(key_of[7], (HID, F * LEV), (F * LEV) ** -0.5, 0.375)
    b_first = gaussian(key_of[8], (HID,), 0.5, 3.0, (), jnp.float32)
    w_second = gaussian(key_of[9], (HID, HID), HID ** -0.5, 0.1875)
    b_second = gaussian(key_of[10], (HID,), 0.5, 3.0, (), jnp.float32)
    w_third = gaussian(key_of[11], (F * LEV, HID), HID ** -0.5, 0.1875)
    b_third = gaussian(key_of[12], (F * LEV,), 0.2, 1.2, (), jnp.float32)
    return dict(state=state, legendre=legendre, lat_weight=lat_weight, modes=modes, mode_rates=mode_rates, diffusion=diffusion, norm_gain=norm_gain, w_first=w_first, b_first=b_first, w_second=w_second, b_second=b_second, w_third=w_third, b_third=b_third)


highest = lax.Precision.HIGHEST
norm_eps = 1e-06

def phase_angles(waves, longitudes):
    wave_idx = jnp.arange(waves, dtype=jnp.int32)
    lon_idx = jnp.arange(longitudes, dtype=jnp.int32)
    phase_turns = wave_idx[:, None] * lon_idx[None, :] % longitudes
    return (2.0 * jnp.pi / longitudes * phase_turns.astype(jnp.float32), wave_idx)

def synthesis_table(waves, longitudes):
    angle_table, wave_idx = phase_angles(waves, longitudes)
    factor = jnp.where(wave_idx == 0, 1.0, 2.0).astype(jnp.float32)[:, None]
    return jnp.stack([factor * jnp.cos(angle_table), -factor * jnp.sin(angle_table)], axis=1)

def analysis_table(waves, longitudes):
    angle_table, wave_idx = phase_angles(waves, longitudes)
    flipped = angle_table.T
    return jnp.stack([jnp.cos(flipped), -jnp.sin(flipped)], axis=2) / longitudes

def column_physics(columns, norm_gain, w_first, b_first, w_second, b_second, w_third, b_third):
    values = columns.astype(jnp.float32)
    inverse_rms = lax.rsqrt(lax.optimization_barrier(jnp.mean(values * values, axis=0, keepdims=True)) + norm_eps)
    normed = (values * inverse_rms * norm_gain[:, None]).astype(jnp.bfloat16)
    hidden_one = jax.nn.gelu(jnp.dot(w_first.astype(jnp.float32), normed.astype(jnp.float32), preferred_element_type=jnp.float32) + b_first[:, None]).astype(jnp.bfloat16)
    hidden_two = jax.nn.gelu(jnp.dot(w_second.astype(jnp.float32), hidden_one.astype(jnp.float32), preferred_element_type=jnp.float32) + b_second[:, None]).astype(jnp.bfloat16)
    return (jnp.dot(w_third.astype(jnp.float32), hidden_two.astype(jnp.float32), preferred_element_type=jnp.float32) + b_third[:, None]).astype(jnp.bfloat16)

def reference(state, legendre, lat_weight, modes, mode_rates, diffusion, norm_gain, w_first, b_first, w_second, b_second, w_third, b_third):
    wave_idx = jnp.arange(M, dtype=jnp.int32)
    degree_index = wave_idx[:, None] + jnp.arange(M, dtype=jnp.int32)[None, :]
    kept_mask = (degree_index < M).astype(jnp.float32)
    kept_basis = legendre * kept_mask[:, None, :]
    band_coeffs = jnp.einsum('flmcj,maj->flmca', state, kept_basis, precision=highest)
    grid_field = jnp.einsum('flmca,mco->flao', band_coeffs, synthesis_table(M, LON), precision=highest)
    grid_low = grid_field.astype(jnp.bfloat16)

    def one_row(row_block):
        flat_cols = row_block.reshape(F * LEV, LON)
        return column_physics(flat_cols, norm_gain, w_first, b_first, w_second, b_second, w_third, b_third).reshape(F, LEV, LON)
    tendency = lax.map(one_row, jnp.moveaxis(grid_low, 2, 0))
    tendency = jnp.moveaxis(tendency, 0, 2)
    updated = (grid_field + tendency.astype(jnp.float32)) * lat_weight[None, None, :, None]
    wave_coeffs = jnp.einsum('flao,omc->flmca', updated, analysis_table(M, LON), precision=highest)
    spectral = jnp.einsum('flmca,maj->flmcj', wave_coeffs, kept_basis, precision=highest)
    growth = (degree_index * (degree_index + 1)).astype(jnp.float32)
    amplitude = jnp.einsum('lk,lmcj->kmcj', modes, spectral[1], precision=highest)
    amplitude = amplitude / (1.0 + mode_rates[:, None, None, None] * growth[None, :, None, :])
    solved = jnp.einsum('lk,kmcj->lmcj', modes, amplitude, precision=highest)
    combined = jnp.concatenate([spectral[:1], solved[None], spectral[2:]], axis=0)
    scaled_growth = growth / (M * (M - 1))
    damping = 1.0 + diffusion[:, None, None] * (scaled_growth * scaled_growth)[None]
    return combined / damping[:, None, :, None, :]
```

```python
import jax
import jax.numpy as jnp
import numpy as np
from jax import lax
from jax.experimental import pallas as pl
from jax.experimental.pallas import tpu as pltpu
from jax.sharding import PartitionSpec as P

F, LEV, M, LAT, LON, HID = 4, 64, 256, 384, 768, 1024
HALF = LON // 2
EPS = 1e-06
LOGICAL = pl.DeviceIdType.LOGICAL
bf16, f32 = jnp.bfloat16, jnp.float32


def tables():
    b = np.arange(4)[:, None]
    r = np.arange(128)[None, :]
    m = (8 * (r // 4) + 2 * (r % 4) + b // 2).reshape(-1)
    c = np.broadcast_to(b % 2, (4, 128)).reshape(-1)
    o = np.arange(HALF)
    angle = 2.0 * np.pi * ((m[:, None] * o[None, :]) % LON) / LON
    wave = np.where(c[:, None] == 0, np.cos(angle), -np.sin(angle))
    inverse = (np.where(m == 0, 1.0, 2.0)[:, None] * wave).T.astype(np.float32)
    forward = (wave / LON).astype(np.float32)
    parts = []
    for t in (inverse, forward):
        hi = t.astype(jnp.bfloat16)
        parts += [hi, (t - hi.astype(np.float32)).astype(jnp.bfloat16)]
    return parts


def split(x):
    hi = x.astype(bf16)
    return hi, (x - hi.astype(f32)).astype(bf16)


def nn(a, b):
    return lax.dot_general(a, b, (((1,), (0,)), ((), ())), preferred_element_type=f32)


def nt(a, b):
    return lax.dot_general(a, b, (((1,), (1,)), ((), ())), preferred_element_type=f32)


def place():
    w, i = lax.axis_index("wave"), lax.axis_index("level")
    return w, i, w // 8, (w // 2) % 4, w % 2


def wave_peers(x, z):
    xs = [(x + d) % 4 for d in range(4)]
    zs = [(z + d) % 4 for d in range(4)]
    for dz in (2, 1, 3, 0):
        for dx in (2, 1, 3, 0):
            for core in (0, 1):
                yield dx == 0 and dz == 0, core, xs[dx] * 8 + zs[dz] * 2 + core


def meet(w, i, core, x, z):
    barrier = pltpu.get_barrier_semaphore()
    for d in range(1, 8):
        pl.semaphore_signal(barrier, inc=1, device_id=w * 8 + (i + d) % 8, device_id_type=LOGICAL)
    for own_chip, pc, pw in wave_peers(x, z):
        if own_chip:
            continue
        pl.semaphore_signal(barrier, inc=1, device_id=pw * 8 + i, device_id_type=LOGICAL)
    pl.semaphore_signal(barrier, inc=1, device_id=(w + 1 - 2 * core) * 8 + i, device_id_type=LOGICAL)
    return barrier


def block_transpose(v):
    lane = lax.broadcasted_iota(jnp.int32, v[0].shape, 1)
    low, even = lane < 64, (lane % 64) < 32
    l02 = jnp.where(low, v[0], pltpu.roll(v[2], 64, 1))
    h02 = jnp.where(low, pltpu.roll(v[0], 64, 1), v[2])
    l13 = jnp.where(low, v[1], pltpu.roll(v[3], 64, 1))
    h13 = jnp.where(low, pltpu.roll(v[1], 64, 1), v[3])
    return [
        jnp.where(even, l02, pltpu.roll(l13, 32, 1)),
        jnp.where(even, pltpu.roll(l02, 96, 1), l13),
        jnp.where(even, h02, pltpu.roll(h13, 32, 1)),
        jnp.where(even, pltpu.roll(h02, 96, 1), h13),
    ]


def to_grid_kernel(state, leg, lw, x_out, lw_out, leg_v, band, tmp, pa, r1, leg_sem, own_sem, s1, v1, s2, v2, s3, v3):
    w, i, x, z, core = place()
    p = w // 2
    barrier = meet(w, i, core, x, z)
    for m in range(8):
        pltpu.make_async_copy(leg.at[m], leg_v.at[m], leg_sem.at[m]).start()
    col = lax.broadcasted_iota(jnp.int32, (64, M), 1)

    def pair(q, carry):
        acc = jnp.zeros((LAT, 128), f32)
        for h in range(2):
            m = 2 * q + h
            s = jnp.concatenate([state[:, :, m, c, :].reshape(32, M) for c in range(2)], axis=0)
            s = jnp.where(col < M - (8 * w + m), s, 0.0)
            hi, lo = split(s)
            zero = jnp.zeros_like(hi)
            order = (hi, zero, lo, zero) if h == 0 else (zero, hi, zero, lo)
            right = jnp.concatenate(order, axis=0)
            pltpu.make_async_copy(leg.at[m], leg_v.at[m], leg_sem.at[m]).wait()
            bhi, blo = split(leg_v[m])
            both = nt(bhi, right)
            acc += both[:, :128] + both[:, 128:] + nt(blo, right[:128])
        band[q] = acc
        return carry

    lax.fori_loop(0, 4, pair, 0)

    def pack(k, carry):
        for q in range(4):
            tmp[pl.ds(q, 24, stride=4), :] = band[q, pl.ds(pl.multiple_of(24 * k, 8), 24), :]
        pa[k] = tmp[...].reshape(8, 3, 4, 128)
        return carry

    lax.fori_loop(0, 16, pack, 0)

    @pl.when(core == 1)
    def _():
        x_out[:, :, 1] = jnp.zeros((32, 8, 4, 128), f32)

    pl.semaphore_wait(barrier, 38)
    weights = pltpu.make_async_remote_copy(
        lw, lw_out.at[core], s3, v3, device_id=(w + 1 - 2 * core) * 8 + i, device_id_type=LOGICAL
    )
    weights.start()
    own_w = pltpu.make_async_copy(lw, lw_out.at[core], own_sem.at[2])
    own_w.start()
    first = []
    for d in (4, 2, 6, 3, 5, 1, 7):
        pi = (i + d) % 8
        first.append(
            pltpu.make_async_remote_copy(
                pa.at[:, pi], r1.at[i], s1.at[d], v1.at[d], device_id=w * 8 + pi, device_id_type=LOGICAL
            )
        )
        first[-1].start()
    own = pltpu.make_async_copy(pa.at[:, i], r1.at[i], own_sem.at[0])
    own.start()
    own.wait()
    for copy in first:
        copy.wait()

    def out_copy(pc, pw, k):
        lats = r1.at[:, pw // 2, pl.ds(0, 2)] if pc == 0 else r1.at[:, pw // 2, pl.ds(2, 1)]
        goal = x_out.at[w] if pc == 0 else x_out.at[w, :, pl.ds(0, 1)]
        return pltpu.make_async_remote_copy(
            lats, goal, s2.at[k], v2.at[w], device_id=pw * 8 + i, device_id_type=LOGICAL
        )

    peers = list(wave_peers(x, z))
    for k, (own_chip, pc, pw) in enumerate(peers):
        if own_chip:

            @pl.when(core != pc)
            def _(pc=pc, pw=pw, k=k):
                out_copy(pc, pw, k).start()
        else:
            out_copy(pc, pw, k).start()

    def own_copy(pc):
        lats = r1.at[:, p, pl.ds(0, 2)] if pc == 0 else r1.at[:, p, pl.ds(2, 1)]
        goal = x_out.at[w] if pc == 0 else x_out.at[w, :, pl.ds(0, 1)]
        return pltpu.make_async_copy(lats, goal, own_sem.at[1])

    for pc in range(2):

        @pl.when(core == pc)
        def _(pc=pc):
            mine = own_copy(pc)
            mine.start()
            mine.wait()

    weights.wait()
    own_w.wait()
    for k, (own_chip, pc, pw) in enumerate(peers):
        if own_chip:

            @pl.when(core != pc)
            def _(pc=pc, pw=pw, k=k):
                out_copy(pc, pw, k).wait_send()
        else:
            out_copy(pc, pw, k).wait_send()
    for mc in range(2):

        @pl.when(core == mc)
        def _(mc=mc):
            for own_chip, pc, pw in peers:
                if own_chip and pc == mc:
                    continue
                goal = x_out.at[pw] if mc == 0 else x_out.at[pw, :, pl.ds(0, 1)]
                lats = r1.at[:, p, pl.ds(0, 2)] if mc == 0 else r1.at[:, p, pl.ds(2, 1)]
                pltpu.make_async_remote_copy(
                    lats, goal, s2.at[0], v2.at[pw], device_id=pw * 8 + i, device_id_type=LOGICAL
                ).wait_recv()


def gelu(x):
    return jax.nn.gelu(x)


def physics_kernel(
    xr, lw, inv_hi, inv_lo, fwd_hi, fwd_lo, gain, w1, b1, w2, b2, w3, b3, yo, w1p, w3p, xt, xl, s_hi, s_lo, d_hi, d_lo
):
    w, i, x, z, core = place()
    row = lax.broadcasted_iota(jnp.int32, (256, 256), 0)
    lane = lax.broadcasted_iota(jnp.int32, (256, 256), 1)
    source = ((lane // 8) % 4) * 64 + (lane // 32) * 8 + lane % 8
    w1p[...] = nn(w1[...], (row == source).astype(bf16)).astype(bf16)
    for k in range(8):
        for f in range(4):
            w3p[k * 32 + f * 8 : k * 32 + f * 8 + 8, :] = w3[f * 64 + k * 8 : f * 64 + k * 8 + 8, :]

    def one_lat(a, carry):
        e = 3 * i + jnp.where(core == 0, a, 2)
        at = lax.broadcasted_iota(jnp.int32, (2, 1, 128), 0) * 12 + lax.broadcasted_iota(jnp.int32, (2, 1, 128), 2)
        inside = lax.broadcasted_iota(jnp.int32, (2, 1, 128), 2) < 12
        weight = jnp.sum(jnp.where((at == e) & inside, lw[...], 0.0))
        for g in range(2):
            v = [xr[:, 4 * g + k, a].reshape(128, 128) for k in range(4)]
            for b, t in enumerate(block_transpose(v)):
                here = (slice(b * 128, (b + 1) * 128), slice(g * 128, (g + 1) * 128))
                xt[here], xl[here] = split(t)

        def columns(k, carry):
            rows = pl.ds(pl.multiple_of(k * 128, 128), 128)
            even = nn(inv_hi[rows, :256], xt[:256, :]) + nn(inv_lo[rows, :256], xt[:256, :]) + nn(inv_hi[rows, :256], xl[:256, :])
            odd = nn(inv_hi[rows, 256:], xt[256:, :]) + nn(inv_lo[rows, 256:], xt[256:, :]) + nn(inv_hi[rows, 256:], xl[256:, :])
            grid = jnp.concatenate([even + odd, even - odd], axis=0)
            v = grid.astype(bf16).astype(f32)
            scale = lax.rsqrt(jnp.mean(v * v, axis=1, keepdims=True) + EPS)
            n = (v * scale * gain[...]).astype(bf16)
            h = gelu(nt(n, w1p[...]) + b1[...]).astype(bf16)
            h = gelu(nt(h, w2[...]) + b2[...]).astype(bf16)
            t = (nt(h, w3p[...]) + b3[...]).astype(bf16)
            u = (grid + t.astype(f32)) * weight
            s_hi[rows, :], s_lo[rows, :] = split(u[:128] + u[128:])
            d_hi[rows, :], d_lo[rows, :] = split(u[:128] - u[128:])
            return carry

        lax.fori_loop(0, 3, columns, 0)
        even = nn(fwd_hi[:256], s_hi[...]) + nn(fwd_hi[:256], s_lo[...]) + nn(fwd_lo[:256], s_hi[...])
        odd = nn(fwd_hi[256:], d_hi[...]) + nn(fwd_hi[256:], d_lo[...]) + nn(fwd_lo[256:], d_hi[...])
        y = (even[:128], even[128:], odd[:128], odd[128:])
        for g in range(2):
            for k, t in enumerate(block_transpose([v[:, g * 128 : (g + 1) * 128] for v in y])):
                yo[:, a, 4 * g + k] = t.reshape(32, 4, 128)
        return carry

    lax.fori_loop(0, 2, one_lat, 0)


def to_spectral_kernel(
    yo, leg, modes, modes_t, rates, diff, diff1, out, leg_v, r2, vr, vs, vt, vl, f1, g1, hs, qs, leg_sem, own_sem, s1, v1, s2, v2, s3, v3, s4, v4
):
    w, i, x, z, core = place()
    p = w // 2
    barrier = meet(w, i, core, x, z)
    for m in range(8):
        pltpu.make_async_copy(leg.at[m], leg_v.at[m], leg_sem.at[m]).start()
    pl.semaphore_wait(barrier, 38)
    peers = list(wave_peers(x, z))

    def lats(mc, pw):
        return yo.at[pw] if mc == 0 else yo.at[pw, pl.ds(0, 1)]

    def goal(mc, chip):
        return r2.at[chip, pl.ds(0, 2)] if mc == 0 else r2.at[chip, pl.ds(2, 1)]

    def send(mc, pw, k):
        return pltpu.make_async_remote_copy(
            lats(mc, pw), goal(mc, p), s1.at[k], v1.at[w], device_id=pw * 8 + i, device_id_type=LOGICAL
        )

    for mc in range(2):

        @pl.when(core == mc)
        def _(mc=mc):
            for k, (own_chip, pc, pw) in enumerate(peers):
                if not (own_chip and pc == mc):
                    send(mc, pw, k).start()
            mine = pltpu.make_async_copy(lats(mc, w), goal(mc, p), own_sem.at[0])
            mine.start()
            mine.wait()
            for k, (own_chip, pc, pw) in enumerate(peers):
                if not (own_chip and pc == mc):
                    send(mc, pw, k).wait_send()

    for own_chip, pc, pw in peers:

        def arrived(pc=pc, pw=pw):
            pltpu.make_async_remote_copy(
                lats(pc, pw), goal(pc, pw // 2), s1.at[0], v1.at[pw], device_id=pw * 8 + i, device_id_type=LOGICAL
            ).wait_recv()

        if own_chip:
            pl.when(core != pc)(arrived)
        else:
            arrived()

    second = []
    for d in (4, 2, 6, 3, 5, 1, 7):
        pi = (i + d) % 8
        second.append(
            pltpu.make_async_remote_copy(
                r2.at[:, :, pi], vr.at[:, i], s2.at[d], v2.at[d], device_id=w * 8 + pi, device_id_type=LOGICAL
            )
        )
        second[-1].start()
    own = pltpu.make_async_copy(r2.at[:, :, i], vr.at[:, i], own_sem.at[1])
    own.start()
    own.wait()
    for copy in second:
        copy.wait()

    def unpack(k, carry):
        vs[pl.ds(pl.multiple_of(96 * k, 8), 96), :] = vr[k].reshape(96, 128)
        return carry

    lax.fori_loop(0, 16, unpack, 0)
    for q in range(4):
        vt[q], vl[q] = split(vs[pl.ds(q, LAT, stride=4), :].T)

    col = lax.broadcasted_iota(jnp.int32, (64, M), 1)

    def damping(n, strength):
        g = (n * (n + 1)).astype(f32) / (M * (M - 1))
        return 1.0 + strength * (g * g)

    def pair(q, carry):
        for h in range(2):
            m = 2 * q + h
            pltpu.make_async_copy(leg.at[m], leg_v.at[m], leg_sem.at[m]).wait()
            bhi, blo = split(leg_v[m])
            left, rest = vt[q, h * 64 : (h + 1) * 64, :], vl[q, h * 64 : (h + 1) * 64, :]
            n = 8 * w + m + col
            spec = jnp.where(n < M, nn(left, bhi) + nn(left, blo) + nn(rest, bhi), 0.0)
            out[m] = spec / damping(n, diff[...])
            for c in range(2):
                f1[m, c] = spec[c * 32 + 8 : c * 32 + 16, :]
        return carry

    lax.fori_loop(0, 4, pair, 0)

    third = []
    for d in (4, 2, 6, 3, 5, 1, 7):
        pi = (i + d) % 8
        third.append(
            pltpu.make_async_remote_copy(
                f1.at[pi],
                g1.at[:, pl.ds(pl.multiple_of(8 * i, 8), 8), :],
                s3.at[d],
                v3.at[d],
                device_id=w * 8 + pi,
                device_id_type=LOGICAL,
            )
        )
        third[-1].start()
    own = pltpu.make_async_copy(f1.at[i], g1.at[:, pl.ds(pl.multiple_of(8 * i, 8), 8), :], own_sem.at[2])
    own.start()
    own.wait()
    for copy in third:
        copy.wait()
    n = 8 * w + i + col
    divisor = 1.0 + rates[...] * (n * (n + 1)).astype(f32)
    for c in range(2):
        amplitude = jnp.dot(modes_t[...], g1[c], precision=lax.Precision.HIGHEST, preferred_element_type=f32)
        solved = jnp.dot(modes[...], amplitude / divisor, precision=lax.Precision.HIGHEST, preferred_element_type=f32)
        hs[c] = solved / damping(n, diff1[...])
    fourth = []
    for d in (4, 2, 6, 3, 5, 1, 7):
        pi = (i + d) % 8
        fourth.append(
            pltpu.make_async_remote_copy(
                hs.at[:, pl.ds(pl.multiple_of(8 * pi, 8), 8), :],
                qs.at[i],
                s4.at[d],
                v4.at[d],
                device_id=w * 8 + pi,
                device_id_type=LOGICAL,
            )
        )
        fourth[-1].start()
    own = pltpu.make_async_copy(hs.at[:, pl.ds(pl.multiple_of(8 * i, 8), 8), :], qs.at[i], own_sem.at[3])
    own.start()
    own.wait()
    for copy in fourth:
        copy.wait()
    for m in range(8):
        for c in range(2):
            out[m, c * 32 + 8 : c * 32 + 16, :] = qs[m, c]


VMEM = pl.BlockSpec(memory_space=pltpu.VMEM)
ANY = pl.BlockSpec(memory_space=pl.ANY)
DMA = pltpu.SemaphoreType.DMA


def grid_order(v):
    return v.reshape(F, 8, 8).transpose(1, 0, 2).reshape(1, F * LEV)


def body(state, legendre, lat_weight, modes, mode_rates, diffusion, norm_gain, w_first, b_first, w_second, b_second, w_third, b_third):
    inv_hi, inv_lo, fwd_hi, fwd_lo = [jnp.asarray(t) for t in tables()]
    lw = jnp.pad(lat_weight, (0, 116)).reshape(1, 128)
    x, lw2 = pl.pallas_call(
        to_grid_kernel,
        name="to_grid",
        out_shape=(jax.ShapeDtypeStruct((32, 8, 2, 4, 128), f32), jax.ShapeDtypeStruct((2, 1, 128), f32)),
        in_specs=[VMEM, ANY, VMEM],
        out_specs=(VMEM, VMEM),
        scratch_shapes=[
            pltpu.VMEM((8, LAT, M), f32),
            pltpu.VMEM((4, LAT, 128), f32),
            pltpu.VMEM((96, 128), f32),
            pltpu.VMEM((16, 8, 3, 4, 128), f32),
            pltpu.VMEM((8, 16, 3, 4, 128), f32),
            DMA((8,)), DMA((3,)), DMA((8,)), DMA((8,)), DMA((32,)), DMA((32,)), DMA, DMA,
        ],
        compiler_params=pltpu.CompilerParams(collective_id=0, has_side_effects=True),
    )(state, legendre, lw)
    y = pl.pallas_call(
        physics_kernel,
        name="physics",
        out_shape=jax.ShapeDtypeStruct((32, 2, 8, 4, 128), f32),
        in_specs=[VMEM] * 13,
        out_specs=VMEM,
        scratch_shapes=[
            pltpu.VMEM((HID, 256), bf16),
            pltpu.VMEM((256, HID), bf16),
            pltpu.VMEM((512, 256), bf16),
            pltpu.VMEM((512, 256), bf16),
            pltpu.VMEM((HALF, 256), bf16),
            pltpu.VMEM((HALF, 256), bf16),
            pltpu.VMEM((HALF, 256), bf16),
            pltpu.VMEM((HALF, 256), bf16),
        ],
    )(
        x, lw2, inv_hi, inv_lo, fwd_hi, fwd_lo, grid_order(norm_gain), w_first, b_first.reshape(1, HID),
        w_second, b_second.reshape(1, HID), w_third, grid_order(b_third),
    )
    diff = jnp.broadcast_to(diffusion[None, :, None], (2, F, 8)).reshape(64, 1)
    out = pl.pallas_call(
        to_spectral_kernel,
        name="to_spectral",
        out_shape=jax.ShapeDtypeStruct((8, 64, M), f32),
        in_specs=[VMEM, ANY, VMEM, VMEM, VMEM, VMEM, VMEM],
        out_specs=VMEM,
        scratch_shapes=[
            pltpu.VMEM((8, LAT, M), f32),
            pltpu.VMEM((16, 3, 8, 4, 128), f32),
            pltpu.VMEM((16, 8, 3, 4, 128), f32),
            pltpu.VMEM((1536, 128), f32),
            pltpu.VMEM((4, 128, LAT), bf16),
            pltpu.VMEM((4, 128, LAT), bf16),
            pltpu.VMEM((8, 2, 8, M), f32),
            pltpu.VMEM((2, 64, M), f32),
            pltpu.VMEM((2, 64, M), f32),
            pltpu.VMEM((8, 2, 8, M), f32),
            DMA((8,)), DMA((4,)), DMA((32,)), DMA((32,)), DMA((8,)), DMA((8,)), DMA((8,)), DMA((8,)), DMA((8,)), DMA((8,)),
        ],
        compiler_params=pltpu.CompilerParams(collective_id=1, has_side_effects=True),
    )(y, legendre, modes, modes.T, mode_rates.reshape(LEV, 1), diff, diffusion[1].reshape(1, 1))
    return out.reshape(8, 2, F, 8, M).transpose(2, 3, 0, 1, 4)


def solution(mesh):
    return jax.shard_map(
        body,
        mesh=mesh,
        in_specs=(P(None, "level", "wave", None, None), P("wave", None, None), P("wave")) + (P(),) * 10,
        out_specs=P(None, "level", "wave", None, None),
        check_vma=False,
    )
```

```python
import jax
import jax.numpy as jnp
import numpy as np
from jax import lax
from jax.experimental import pallas as pl
from jax.experimental.pallas import tpu as pltpu
from jax.sharding import PartitionSpec as P

F, LEV, M, LAT, LON, HID = 4, 64, 256, 384, 768, 1024
HALF = LON // 2
EPS = 1e-06
LOGICAL = pl.DeviceIdType.LOGICAL
bf16, f32 = jnp.bfloat16, jnp.float32


def tables():
    b = np.arange(4)[:, None]
    r = np.arange(128)[None, :]
    m = (8 * (r // 4) + 2 * (r % 4) + b // 2).reshape(-1)
    c = np.broadcast_to(b % 2, (4, 128)).reshape(-1)
    o = np.arange(HALF)
    angle = 2.0 * np.pi * ((m[:, None] * o[None, :]) % LON) / LON
    wave = np.where(c[:, None] == 0, np.cos(angle), -np.sin(angle))
    inverse = (np.where(m == 0, 1.0, 2.0)[:, None] * wave).T.astype(np.float32)
    forward = (wave / LON).astype(np.float32)
    parts = []
    for t in (inverse, forward):
        hi = t.astype(jnp.bfloat16)
        parts += [hi, (t - hi.astype(np.float32)).astype(jnp.bfloat16)]
    return parts


def split(x):
    hi = x.astype(bf16)
    return hi, (x - hi.astype(f32)).astype(bf16)


def encode(x):
    hi = x.astype(bf16).astype(f32)
    size = jnp.abs(hi)
    r = jnp.where(size > 0.0, (x - hi) / size, 0.0)
    return hi, jnp.clip(jnp.floor(r * 2048.0 + 8.0), 0.0, 15.0)


def decode(hi, k):
    return hi + jnp.abs(hi) * ((k - 7.5) * (1.0 / 2048.0))


def gelu(x):
    c = 0.7978845608028654
    half = 0.5 * x
    return half + half * jnp.tanh(x * (c + (c * 0.044715) * (x * x)))


def nn(a, b):
    return lax.dot_general(a, b, (((1,), (0,)), ((), ())), preferred_element_type=f32)


def nt(a, b):
    return lax.dot_general(a, b, (((1,), (1,)), ((), ())), preferred_element_type=f32)


def block_transpose(v):
    lane = lax.broadcasted_iota(jnp.int32, v[0].shape, 1)
    low, even = lane < 64, (lane % 64) < 32
    l02 = jnp.where(low, v[0], pltpu.roll(v[2], 64, 1))
    h02 = jnp.where(low, pltpu.roll(v[0], 64, 1), v[2])
    l13 = jnp.where(low, v[1], pltpu.roll(v[3], 64, 1))
    h13 = jnp.where(low, pltpu.roll(v[1], 64, 1), v[3])
    return [
        jnp.where(even, l02, pltpu.roll(l13, 32, 1)),
        jnp.where(even, pltpu.roll(l02, 96, 1), l13),
        jnp.where(even, h02, pltpu.roll(h13, 32, 1)),
        jnp.where(even, pltpu.roll(h02, 96, 1), h13),
    ]


class Place:
    def __init__(self):
        self.w, self.i = lax.axis_index("wave"), lax.axis_index("level")
        w, i = self.w, self.i
        self.p, self.core, self.y, self.zl = w // 2, w % 2, i // 2, i % 2
        x, z = w // 8, ((w // 2) % 4) * 2 + i % 2
        self.xs = [(x + d) % 4 for d in range(4)]
        self.zs = [(z + d) % 8 for d in range(8)]
        self.ys = [(self.y + d) % 4 for d in range(4)]

    def plane(self):
        for dz in (4, 3, 5, 2, 6, 1, 7, 0):
            for dx in (2, 1, 3, 0):
                zh, zl = self.zs[dz] // 2, self.zs[dz] % 2
                p = self.xs[dx] * 4 + zh
                for core in (0, 1):
                    yield dz == 0 and dx == 0, core, p, zl, p * 16 + core * 8 + self.y * 2 + zl

    def level(self):
        for d in (4, 2, 6, 3, 5, 1, 7):
            i = (self.i + d) % 8
            yield d, i, self.w * 8 + i

    def column(self):
        for d in (2, 1, 3):
            yield d, self.ys[d], self.w * 8 + self.ys[d] * 2 + self.zl


def remote(src, dst, send, recv, device):
    return pltpu.make_async_remote_copy(src, dst, send, recv, device_id=device, device_id_type=LOGICAL)


def meet(at):
    barrier = pltpu.get_barrier_semaphore()
    for d, i, device in at.level():
        pl.semaphore_signal(barrier, inc=1, device_id=device, device_id_type=LOGICAL)
    buddy = (at.w + 1 - 2 * at.core) * 8 + at.i
    pl.semaphore_signal(barrier, inc=1, device_id=buddy, device_id_type=LOGICAL)
    for dz in (4, 3, 5, 2, 6, 1, 7, 0):
        for dx in (2, 1, 3, 0):
            if dz == 0 and dx == 0:
                continue
            zh, zl = at.zs[dz] // 2, at.zs[dz] % 2
            for core in (0, 1):
                device = ((at.xs[dx] * 4 + zh) * 2 + core) * 8 + at.y * 2 + zl
                pl.semaphore_signal(barrier, inc=1, device_id=device, device_id_type=LOGICAL)
    return barrier, 7 + 1 + 62 + 0


def legendre_forward(at, r):
    w = at.w
    col = lax.broadcasted_iota(jnp.int32, (64, M), 1)

    def pair(q, carry):
        acc = jnp.zeros((LAT, 128), f32)
        for h in range(2):
            m = 2 * q + h
            s = jnp.concatenate([r.state[:, :, m, c, :].reshape(32, M) for c in range(2)], axis=0)
            s = jnp.where(col < M - (8 * w + m), s, 0.0)
            hi, lo = split(s)
            zero = jnp.zeros_like(hi)
            order = (hi, zero, lo, zero) if h == 0 else (zero, hi, zero, lo)
            right = jnp.concatenate(order, axis=0)
            pltpu.make_async_copy(r.leg.at[m], r.leg_v.at[m], r.leg_sem.at[m]).wait()
            bhi, blo = split(r.leg_v[m])
            r.leg_hi[m] = bhi
            r.leg_lo[m] = blo
            both = nt(bhi, right)
            acc += both[:, :128] + both[:, 128:] + nt(blo, right[:128])
        r.band[q] = acc
        return carry

    lax.fori_loop(0, 4, pair, 0)

    def pack(k, carry):
        code = []
        for q in range(4):
            hi, step = encode(r.band[q, pl.ds(pl.multiple_of(24 * k, 8), 24), :])
            r.tmp[pl.ds(q, 24, stride=4), :] = hi
            code.append(step)
        r.tmc[pl.ds(0, 24, stride=2), :] = 16.0 * code[0] + code[1]
        r.tmc[pl.ds(1, 24, stride=2), :] = 16.0 * code[2] + code[3]
        hi = r.tmp[...].reshape(4, 2, 3, 4, 128).astype(bf16)
        low = r.tmc[...].reshape(4, 2, 3, 2, 128).astype(bf16)
        for t in range(3):
            r.pa[t, :, pl.ds(2 * k, 2)] = hi[:, :, t]
            r.ca[t, :, pl.ds(2 * k, 2)] = low[:, :, t]
        return carry

    lax.fori_loop(0, 16, pack, 0)


def along_y_start(at, t, pairs, send, recv, own_sem):
    for n, (src, dst) in enumerate(pairs):
        for d, y, device in at.column():
            remote(src.at[t, y], dst.at[t, at.y], send.at[n, t], recv.at[n, t], device).start()
        pltpu.make_async_copy(src.at[t, at.y], dst.at[t, at.y], own_sem.at[n, t]).start()


def along_y_wait(at, t, pairs, send, recv, own_sem):
    for n, (src, dst) in enumerate(pairs):
        remote(src.at[t, pl.ds(0, 3)], dst.at[t, pl.ds(0, 3)], send.at[n, t], recv.at[n, t], 0).wait()
        pltpu.make_async_copy(src.at[t, at.y], dst.at[t, at.y], own_sem.at[n, t]).wait()


def to_grid_start(at, r, t):
    core, a = (0, t) if t < 2 else (1, 0)
    me = at.w * 2 + at.zl
    for n, (src, dst) in enumerate(((r.r1, r.xh), (r.c1, r.xc))):
        for chip, pc, p, zl, device in at.plane():
            if pc != core:
                continue
            piece, goal = src.at[t, :, p * 2 + zl], dst.at[a, me]
            copy = remote(piece, goal, r.s2.at[n, t], r.v2.at[n, a], device)
            if chip:
                pl.when(at.core != core)(lambda copy=copy: copy.start())
            else:
                copy.start()
        own = pltpu.make_async_copy(src.at[t, :, at.p * 2 + at.zl], dst.at[a, me], r.own_sem.at[n, a])
        pl.when(at.core == core)(lambda own=own: own.start())


def to_grid_arrived(at, r, a):
    me = at.w * 2 + at.zl
    for n, (src, dst) in enumerate(((r.r1, r.xh), (r.c1, r.xc))):
        some = dst.at[a, pl.ds(0, 63)]
        remote(some, some, r.s2.at[n, 0], r.v2.at[n, a], 0).wait_recv()
        pltpu.make_async_copy(src.at[0, :, 0], dst.at[a, me], r.own_sem.at[n, a]).wait()


def to_grid_sent(at, r, t):
    for n, src in enumerate((r.r1, r.c1)):
        for core in range(2):
            pieces = 31 if core == (0 if t < 2 else 1) else 32

            @pl.when(at.core == core)
            def _(n=n, src=src, pieces=pieces):
                some = src.at[t, :, pl.ds(0, pieces)]
                remote(some, some, r.s2.at[n, t], r.v2.at[n, 0], 0).wait_send()


def one_latitude(at, r, a):
    e = 3 * at.i + (a if a else jnp.where(at.core == 0, 0, 2))
    lane12 = lax.broadcasted_iota(jnp.int32, (2, 1, 128), 2)
    number = lax.broadcasted_iota(jnp.int32, (2, 1, 128), 0) * 12 + lane12
    weight = jnp.sum(jnp.where((number == e) & (lane12 < 12), r.lat[...], 0.0))
    for g in range(2):
        v = []
        for k in range(4):
            y, zl = 2 * g + k // 2, k % 2
            code = r.xc.reshape(2, 32, 2, 4, 2, 128)[a, :, zl, y].astype(f32).reshape(64, 128)
            first = jnp.floor(code * (1.0 / 16.0))
            r.steps[k, pl.ds(0, 64, stride=2), :] = first
            r.steps[k, pl.ds(1, 64, stride=2), :] = code - 16.0 * first
            v.append(decode(r.xh.reshape(2, 32, 2, 4, 4, 128)[a, :, zl, y].astype(f32).reshape(128, 128), r.steps[k]))
        for b, t in enumerate(block_transpose(v)):
            here = (slice(b * 128, (b + 1) * 128), slice(g * 128, (g + 1) * 128))
            r.xt[here], r.xl[here] = split(t)

    def inverse(rows, half):
        hi, lo, x, rest = r.ih[rows, half], r.il[rows, half], r.xt[half, :], r.xl[half, :]
        return nn(hi, x) + nn(lo, x) + nn(hi, rest)

    def columns(k, carry):
        rows = pl.ds(pl.multiple_of(k * 128, 128), 128)
        even, odd = inverse(rows, slice(0, 256)), inverse(rows, slice(256, 512))
        grid = jnp.concatenate([even + odd, even - odd], axis=0)
        v = grid.astype(bf16).astype(f32)
        scale = lax.rsqrt(jnp.mean(v * v, axis=1, keepdims=True) + EPS)
        n = (v * scale * r.gain_p[...]).astype(bf16)
        h = gelu(nt(n, r.w1p[...]) + r.b1[...]).astype(bf16)
        h = gelu(nt(h, r.w2v[...]) + r.b2[...]).astype(bf16)
        t = (nt(h, r.w3p[...]) + r.b3p[...]).astype(bf16)
        u = (grid + t.astype(f32)) * weight
        r.s_hi[rows, :], r.s_lo[rows, :] = split(u[:128] + u[128:])
        r.d_hi[rows, :], r.d_lo[rows, :] = split(u[:128] - u[128:])
        return carry

    lax.fori_loop(0, 3, columns, 0)

    def forward(half, hi, lo):
        return nn(r.fh[half, :], hi[...]) + nn(r.fh[half, :], lo[...]) + nn(r.fl[half, :], hi[...])

    even, odd = forward(slice(0, 256), r.s_hi, r.s_lo), forward(slice(256, 512), r.d_hi, r.d_lo)
    y = (even[:128], even[128:], odd[:128], odd[128:])
    for g in range(2):
        for k, t in enumerate(block_transpose([v[:, g * 128 : (g + 1) * 128] for v in y])):
            hi, step = encode(t)
            r.steps[k] = step
            code = 16.0 * r.steps[k, pl.ds(0, 64, stride=2), :] + r.steps[k, pl.ds(1, 64, stride=2), :]
            r.yh.reshape(2, 32, 2, 4, 4, 128)[a, :, k % 2, 2 * g + k // 2] = hi.reshape(32, 4, 128).astype(bf16)
            r.yc.reshape(2, 32, 2, 4, 2, 128)[a, :, k % 2, 2 * g + k // 2] = code.reshape(32, 2, 128).astype(bf16)


def network_weights(r):
    row = lax.broadcasted_iota(jnp.int32, (256, 256), 0)
    lane = lax.broadcasted_iota(jnp.int32, (256, 256), 1)
    pick = row == ((lane // 8) % 4) * 64 + (lane // 32) * 8 + lane % 8
    r.w1p[...] = nn(r.w1v[...], pick.astype(bf16)).astype(bf16)
    for k in range(8):
        for f in range(4):
            r.w3p[k * 32 + f * 8 : k * 32 + f * 8 + 8, :] = r.w3v[f * 64 + k * 8 : f * 64 + k * 8 + 8, :]
    for a, b in ((r.gain, r.gain_p), (r.b3, r.b3p)):
        rows = jnp.broadcast_to(a[...], (8, 256))
        b[...] = jnp.dot(rows, pick.astype(f32), precision=lax.Precision.HIGHEST, preferred_element_type=f32)[:1]


def send_latitude(at, r, a, mc):
    t = a if mc == 0 else 2
    me = at.p * 2 + at.zl
    for n, (src, dst) in enumerate(((r.yh, r.r2), (r.yc, r.c2))):
        for chip, core, p, zl, device in at.plane():
            if not (chip and core == mc):
                piece = src.at[a, (p * 2 + core) * 2 + zl]
                remote(piece, dst.at[t, :, me], r.s3.at[n, a], r.v3.at[n, t], device).start()
        pltpu.make_async_copy(src.at[a, at.w * 2 + at.zl], dst.at[t, :, me], r.own_sem.at[n, a]).start()


def latitude_own(at, r, a):
    for n, (src, dst) in enumerate(((r.yh, r.r2), (r.yc, r.c2))):
        pltpu.make_async_copy(src.at[a, 0], dst.at[0, :, 0], r.own_sem.at[n, a]).wait()


def latitude_sent(at, r, a):
    for n, src in enumerate((r.yh, r.yc)):
        some = src.at[a, pl.ds(0, 63)]
        remote(some, some, r.s3.at[n, a], r.v3.at[n, 0], 0).wait_send()


def wait_latitude(at, r, t):
    for n, dst in enumerate((r.r2, r.c2)):
        for core in range(2):
            pieces = 31 if core == (0 if t < 2 else 1) else 32

            @pl.when(at.core == core)
            def _(n=n, dst=dst, pieces=pieces):
                some = dst.at[t, :, pl.ds(0, pieces)]
                remote(some, some, r.s3.at[n, 0], r.v3.at[n, t], 0).wait_recv()


def legendre_back(at, r):
    def unpack(k, carry):
        hi = jnp.stack([r.vr[t, :, pl.ds(2 * k, 2)].astype(f32) for t in range(3)], axis=2)
        low = jnp.stack([r.vc[t, :, pl.ds(2 * k, 2)].astype(f32) for t in range(3)], axis=2)
        r.vs[pl.ds(pl.multiple_of(96 * k, 8), 96), :] = hi.reshape(96, 128)
        r.vcs[pl.ds(pl.multiple_of(48 * k, 8), 48), :] = low.reshape(48, 128)
        return carry

    lax.fori_loop(0, 16, unpack, 0)
    for q in range(4):
        code = r.vcs[pl.ds(q // 2, LAT, stride=2), :]
        first = jnp.floor(code * (1.0 / 16.0))
        step = first if q % 2 == 0 else code - 16.0 * first
        turned = decode(r.vs[pl.ds(q, LAT, stride=4), :], step).T
        r.vt[q], r.vl[q] = split(turned)
        for h in range(2):
            one = jnp.concatenate([turned[h * 64 + c * 32 + 8 : h * 64 + c * 32 + 16] for c in range(2)], axis=0)
            r.v1t[2 * q + h], r.v1l[2 * q + h] = split(one)
    col = lax.broadcasted_iota(jnp.int32, (64, M), 1)
    field = (lax.broadcasted_iota(jnp.int32, (64, M), 0) // 8) % 4
    strength = jnp.where(
        field == 0, r.diff[0], jnp.where(field == 1, r.diff[1], jnp.where(field == 2, r.diff[2], r.diff[3]))
    )

    def damping(n, strength):
        g = (n * (n + 1)).astype(f32) / (M * (M - 1))
        return 1.0 + strength * (g * g)

    def level_rows(ref, i):
        return ref.at[:, pl.ds(pl.multiple_of(8 * i, 8), 8), :]

    def basis(left, rest, m):
        n = 8 * at.w + m + col[: left.shape[0]]
        spec = nn(left, r.leg_hi[m]) + nn(left, r.leg_lo[m]) + nn(rest, r.leg_hi[m])
        return n, jnp.where(n < M, spec, 0.0)

    def field_one(m, carry):
        n, spec = basis(r.v1t[m], r.v1l[m], m)
        for c in range(2):
            r.f1[m, c] = spec[c * 8 : c * 8 + 8]
        return carry

    lax.fori_loop(0, 8, field_one, 0)
    for d, i, device in at.level():
        remote(r.f1.at[i], level_rows(r.g1, at.i), r.s5, r.v5, device).start()
    own = pltpu.make_async_copy(r.f1.at[at.i], level_rows(r.g1, at.i), r.own_sem.at[0, 0])
    own.start()

    def pair(q, carry):
        for h in range(2):
            m = 2 * q + h
            n, spec = basis(r.vt[q, h * 64 : (h + 1) * 64, :], r.vl[q, h * 64 : (h + 1) * 64, :], m)
            done = spec / damping(n, strength)
            for c in range(2):
                r.out[:, :, m, c, :] = done[c * 32 : (c + 1) * 32].reshape(F, 8, M)
        return carry

    lax.fori_loop(0, 4, pair, 0)
    own.wait()
    n = 8 * at.w + at.i + col
    row = lax.broadcasted_iota(jnp.int32, (64, 64), 0)
    lane = lax.broadcasted_iota(jnp.int32, (64, 64), 1)
    rates = jnp.sum(jnp.where(row == lane, r.rates[...], 0.0), axis=1, keepdims=True)
    divisor = 1.0 + rates * (n * (n + 1)).astype(f32)
    damp = damping(n, r.diff[1])
    remote(r.f1.at[pl.ds(0, 7)], r.g1.at[:, pl.ds(0, 56), :], r.s5, r.v5, 0).wait_recv()
    for c in range(2):
        amplitude = lax.dot_general(
            r.modes[...], r.g1[c], (((0,), (0,)), ((), ())), precision=lax.Precision.HIGHEST, preferred_element_type=f32
        )
        solved = jnp.dot(
            r.modes[...], amplitude / divisor, precision=lax.Precision.HIGHEST, preferred_element_type=f32
        )
        r.hs[c] = solved / damp
    for d, i, device in at.level():
        remote(level_rows(r.hs, i), r.qs.at[at.i], r.s6, r.v6, device).start()
    own = pltpu.make_async_copy(level_rows(r.hs, at.i), r.qs.at[at.i], r.own_sem.at[1, 0])
    own.start()
    own.wait()
    remote(r.f1.at[pl.ds(0, 7)], r.g1.at[:, pl.ds(0, 56), :], r.s5, r.v5, 0).wait_send()
    remote(r.hs.at[:, pl.ds(0, 56), :], r.qs.at[pl.ds(0, 7)], r.s6, r.v6, 0).wait()
    for m in range(8):
        for c in range(2):
            r.out[1, :, m, c, :] = r.qs[m, c]


INPUTS = ["state_in", "leg", "lw", "modes", "rates", "diff", "gain", "w1", "b1", "w2", "b2", "w3", "b3", "ihh", "ilh", "fhh", "flh"]
DMA = pltpu.SemaphoreType.DMA
SCRATCH = dict(
    state=((F, 8, 8, 2, M), f32), leg_v=((8, LAT, M), f32), leg_hi=((8, LAT, M), bf16), leg_lo=((8, LAT, M), bf16), band=((4, LAT, 128), f32),
    tmp=((96, 128), f32), tmc=((48, 128), f32), pa=((3, 4, 32, 4, 128), bf16), ca=((3, 4, 32, 2, 128), bf16),
    r1=((3, 4, 32, 4, 128), bf16), c1=((3, 4, 32, 2, 128), bf16), xh=((2, 64, 4, 4, 128), bf16),
    xc=((2, 64, 4, 2, 128), bf16), lat=((2, 1, 128), f32), row=((1, 128), f32), w1v=((HID, 256), bf16),
    w2v=((HID, HID), bf16), w3v=((256, HID), bf16), ih=((HALF, 512), bf16), il=((HALF, 512), bf16),
    fh=((512, HALF), bf16), fl=((512, HALF), bf16), w1p=((HID, 256), bf16), w3p=((256, HID), bf16),
    gain_p=((1, 256), f32), b3p=((1, 256), f32), steps=((4, 128, 128), f32), xt=((512, 256), bf16),
    xl=((512, 256), bf16), s_hi=((HALF, 256), bf16), s_lo=((HALF, 256), bf16), d_hi=((HALF, 256), bf16),
    d_lo=((HALF, 256), bf16), yh=((2, 64, 4, 4, 128), bf16), yc=((2, 64, 4, 2, 128), bf16),
    r2=((3, 4, 32, 4, 128), bf16), c2=((3, 4, 32, 2, 128), bf16), vr=((3, 4, 32, 4, 128), bf16),
    vc=((3, 4, 32, 2, 128), bf16), vs=((1536, 128), f32), vcs=((768, 128), f32), vt=((4, 128, LAT), bf16),
    vl=((4, 128, LAT), bf16), f1=((8, 2, 8, M), f32), g1=((2, 64, M), f32), hs=((2, 64, M), f32),
    qs=((8, 2, 8, M), f32), v1t=((8, 16, LAT), bf16), v1l=((8, 16, LAT), bf16),
)
SEMS = dict(
    leg_sem=(8,), load_sem=(8,), own_sem=(2, 2), lat_sem=(3,), y_own=(2, 3), s1=(2, 3), v1=(2, 3), s2=(2, 3), v2=(2, 2),
    s3=(2, 2), v3=(2, 3), s4=(2, 3), v4=(2, 3), s5=(), v5=(), s6=(), v6=(),
)


class Refs:
    pass


def step_kernel(*refs):
    r = Refs()
    for name, ref in zip(INPUTS + ["out"] + list(SCRATCH) + list(SEMS), refs, strict=True):
        setattr(r, name, ref)
    at = Place()
    whole_state = pltpu.make_async_copy(r.state_in, r.state, r.load_sem.at[7])
    whole_state.start()
    pltpu.make_async_copy(r.leg.at[0], r.leg_v.at[0], r.leg_sem.at[0]).start()
    barrier, callers = meet(at)
    for m in range(1, 8):
        pltpu.make_async_copy(r.leg.at[m], r.leg_v.at[m], r.leg_sem.at[m]).start()
    loads = [
        pltpu.make_async_copy(a, b, r.load_sem.at[n])
        for n, (a, b) in enumerate(
            ((r.w1, r.w1v), (r.w3, r.w3v), (r.w2, r.w2v), (r.ihh, r.ih), (r.ilh, r.il), (r.fhh, r.fh), (r.flh, r.fl))
        )
    ]
    for load in loads:
        load.start()
    lane = lax.broadcasted_iota(jnp.int32, (1, 128), 1)
    row = jnp.zeros((1, 128), f32)
    for k in range(12):
        row = jnp.where(lane == k, r.lw[k], row)
    r.row[...] = row
    whole_state.wait()
    with jax.named_scope('legfwd'):
        legendre_forward(at, r)
    with jax.named_scope('barwait'):
        pl.semaphore_wait(barrier, callers)
    weights = remote(r.row, r.lat.at[at.core], r.lat_sem.at[0], r.lat_sem.at[1], (at.w + 1 - 2 * at.core) * 8 + at.i)
    weights.start()
    own = pltpu.make_async_copy(r.row, r.lat.at[at.core], r.lat_sem.at[2])
    own.start()
    sc = jax.named_scope
    order = (0, 2, 1)
    there = (((r.pa, r.r1), (r.ca, r.c1)), r.s1, r.v1, r.y_own)
    back = (((r.r2, r.vr), (r.c2, r.vc)), r.s4, r.v4, r.y_own)
    with sc("y1"):
        for t in order:
            along_y_start(at, t, *there)
        for t in order:
            along_y_wait(at, t, *there)
            to_grid_start(at, r, t)
    with sc("weights"):
        own.wait()
        weights.wait()
        for load in loads:
            load.wait()
        network_weights(r)
    with sc("arrive0"):
        to_grid_arrived(at, r, 0)
    with sc("lat0"):
        one_latitude(at, r, 0)

    @pl.when(at.core == 0)
    def _():
        with sc("send0"):
            send_latitude(at, r, 0, 0)
        with sc("arrive1"):
            to_grid_arrived(at, r, 1)
        with sc("lat1"):
            one_latitude(at, r, 1)
        with sc("send1"):
            send_latitude(at, r, 1, 0)
            latitude_own(at, r, 0)
            latitude_own(at, r, 1)

    @pl.when(at.core == 1)
    def _():
        with sc("send"):
            send_latitude(at, r, 0, 1)
            latitude_own(at, r, 0)

    with sc("y2"):
        for t in order:
            wait_latitude(at, r, t)
            along_y_start(at, t, *back)
        for t in order:
            along_y_wait(at, t, *back)
    with sc("legback"):
        legendre_back(at, r)
    with sc("sent"):
        for t in order:
            to_grid_sent(at, r, t)
        latitude_sent(at, r, 0)
        pl.when(at.core == 0)(lambda: latitude_sent(at, r, 1))


VMEM = pl.BlockSpec(memory_space=pltpu.VMEM)
SMEM = pl.BlockSpec(memory_space=pltpu.SMEM)
ANY = pl.BlockSpec(memory_space=pl.ANY)


def body(state, legendre, lat_weight, modes, mode_rates, diffusion, norm_gain, w_first, b_first, w_second, b_second, w_third, b_third):
    return pl.pallas_call(
        step_kernel,
        name="step",
        out_shape=jax.ShapeDtypeStruct((F, 8, 8, 2, M), f32),
        in_specs=[ANY, ANY, SMEM, VMEM, VMEM, SMEM, VMEM, ANY, VMEM, ANY, VMEM, ANY, VMEM, ANY, ANY, ANY, ANY],
        out_specs=VMEM,
        scratch_shapes=[pltpu.VMEM(*s) for s in SCRATCH.values()] + [DMA(s) if s else DMA for s in SEMS.values()],
        compiler_params=pltpu.CompilerParams(collective_id=0, has_side_effects=True),
    )(
        state, legendre, lat_weight, modes, mode_rates.reshape(1, LEV), diffusion, norm_gain.reshape(1, 256), w_first,
        b_first.reshape(1, HID), w_second, b_second.reshape(1, HID), w_third, b_third.reshape(1, 256),
        *[jnp.asarray(t) for t in tables()],
    )


def solution(mesh):
    return jax.shard_map(
        body,
        mesh=mesh,
        in_specs=(P(None, "level", "wave", None, None), P("wave", None, None), P("wave")) + (P(),) * 10,
        out_specs=P(None, "level", "wave", None, None),
        check_vma=False,
    )
```

```python
import jax
import jax.numpy as jnp
import numpy as np
from jax import lax
from jax.experimental import pallas as pl
from jax.experimental.pallas import tpu as pltpu
from jax.sharding import PartitionSpec as P

F, LEV, M, LAT, LON, HID = 4, 64, 256, 384, 768, 1024
HALF = LON // 2
EPS = 1e-06
LOGICAL = pl.DeviceIdType.LOGICAL
bf16, f32 = jnp.bfloat16, jnp.float32


def tables():
    b = np.arange(4)[:, None]
    r = np.arange(128)[None, :]
    m = (8 * (r // 4) + 2 * (r % 4) + b // 2).reshape(-1)
    c = np.broadcast_to(b % 2, (4, 128)).reshape(-1)
    o = np.arange(HALF)
    angle = 2.0 * np.pi * ((m[:, None] * o[None, :]) % LON) / LON
    wave = np.where(c[:, None] == 0, np.cos(angle), -np.sin(angle))
    inverse = (np.where(m == 0, 1.0, 2.0)[:, None] * wave).T.astype(np.float32)
    forward = (wave / LON).astype(np.float32)
    parts = []
    for t in (inverse, forward):
        hi = t.astype(jnp.bfloat16)
        parts += [hi, (t - hi.astype(np.float32)).astype(jnp.bfloat16)]
    return parts


def split(x):
    hi = x.astype(bf16)
    return hi, (x - hi.astype(f32)).astype(bf16)


def encode(x):
    hi = x.astype(bf16).astype(f32)
    size = jnp.abs(hi)
    r = jnp.where(size > 0.0, (x - hi) / size, 0.0)
    return hi, jnp.clip(jnp.floor(r * 2048.0 + 8.0), 0.0, 15.0)


def decode(hi, k):
    return hi + jnp.abs(hi) * ((k - 7.5) * (1.0 / 2048.0))


def gelu(x):
    c = 0.7978845608028654
    half = 0.5 * x
    return half + half * jnp.tanh(x * (c + (c * 0.044715) * (x * x)))


def nn(a, b):
    return lax.dot_general(a, b, (((1,), (0,)), ((), ())), preferred_element_type=f32)


def nt(a, b):
    return lax.dot_general(a, b, (((1,), (1,)), ((), ())), preferred_element_type=f32)


def block_transpose(v):
    lane = lax.broadcasted_iota(jnp.int32, v[0].shape, 1)
    low, even = lane < 64, (lane % 64) < 32
    l02 = jnp.where(low, v[0], pltpu.roll(v[2], 64, 1))
    h02 = jnp.where(low, pltpu.roll(v[0], 64, 1), v[2])
    l13 = jnp.where(low, v[1], pltpu.roll(v[3], 64, 1))
    h13 = jnp.where(low, pltpu.roll(v[1], 64, 1), v[3])
    return [
        jnp.where(even, l02, pltpu.roll(l13, 32, 1)),
        jnp.where(even, pltpu.roll(l02, 96, 1), l13),
        jnp.where(even, h02, pltpu.roll(h13, 32, 1)),
        jnp.where(even, pltpu.roll(h02, 96, 1), h13),
    ]


class Place:
    def __init__(self):
        self.w, self.i = lax.axis_index("wave"), lax.axis_index("level")
        w, i = self.w, self.i
        self.p, self.core, self.y, self.zl = w // 2, w % 2, i // 2, i % 2
        x, z = w // 8, ((w // 2) % 4) * 2 + i % 2
        self.xs = [(x + d) % 4 for d in range(4)]
        self.zs = [(z + d) % 8 for d in range(8)]
        self.ys = [(self.y + d) % 4 for d in range(4)]

    def plane(self):
        for dz in (4, 3, 5, 2, 6, 1, 7, 0):
            for dx in (2, 1, 3, 0):
                zh, zl = self.zs[dz] // 2, self.zs[dz] % 2
                p = self.xs[dx] * 4 + zh
                for core in (0, 1):
                    yield dz == 0 and dx == 0, core, p, zl, p * 16 + core * 8 + self.y * 2 + zl

    def level(self):
        for d in (4, 2, 6, 3, 5, 1, 7):
            i = (self.i + d) % 8
            yield d, i, self.w * 8 + i

    def column(self):
        for d in (2, 1, 3):
            yield d, self.ys[d], self.w * 8 + self.ys[d] * 2 + self.zl


def remote(src, dst, send, recv, device):
    return pltpu.make_async_remote_copy(src, dst, send, recv, device_id=device, device_id_type=LOGICAL)


def meet(at):
    barrier = pltpu.get_barrier_semaphore()
    for d, i, device in at.level():
        pl.semaphore_signal(barrier, inc=1, device_id=device, device_id_type=LOGICAL)
    buddy = (at.w + 1 - 2 * at.core) * 8 + at.i
    pl.semaphore_signal(barrier, inc=1, device_id=buddy, device_id_type=LOGICAL)
    for dz in (4, 3, 5, 2, 6, 1, 7, 0):
        for dx in (2, 1, 3, 0):
            if dz == 0 and dx == 0:
                continue
            zh, zl = at.zs[dz] // 2, at.zs[dz] % 2
            for core in (0, 1):
                device = ((at.xs[dx] * 4 + zh) * 2 + core) * 8 + at.y * 2 + zl
                pl.semaphore_signal(barrier, inc=1, device_id=device, device_id_type=LOGICAL)
    return barrier, 7 + 1 + 62 + 0


def legendre_forward(at, r):
    w = at.w
    col = lax.broadcasted_iota(jnp.int32, (64, M), 1)

    def pair(q, carry):
        acc = jnp.zeros((LAT, 128), f32)
        for h in range(2):
            m = 2 * q + h
            s = jnp.concatenate([r.state[:, :, m, c, :].reshape(32, M) for c in range(2)], axis=0)
            s = jnp.where(col < M - (8 * w + m), s, 0.0)
            hi, lo = split(s)
            zero = jnp.zeros_like(hi)
            order = (hi, zero, lo, zero) if h == 0 else (zero, hi, zero, lo)
            right = jnp.concatenate(order, axis=0)
            pltpu.make_async_copy(r.leg.at[m], r.leg_v.at[m], r.leg_sem.at[m]).wait()
            bhi, blo = split(r.leg_v[m])
            r.leg_hi[m] = bhi
            r.leg_lo[m] = blo
            both = nt(bhi, right)
            acc += both[:, :128] + both[:, 128:] + nt(blo, right[:128])
        r.band[q] = acc
        return carry

    lax.fori_loop(0, 4, pair, 0)

    def pack(k, carry):
        code = []
        for q in range(4):
            hi, step = encode(r.band[q, pl.ds(pl.multiple_of(24 * k, 8), 24), :])
            r.tmp[pl.ds(q, 24, stride=4), :] = hi
            code.append(step)
        r.tmc[pl.ds(0, 24, stride=2), :] = 16.0 * code[0] + code[1]
        r.tmc[pl.ds(1, 24, stride=2), :] = 16.0 * code[2] + code[3]
        hi = r.tmp[...].reshape(4, 2, 3, 4, 128).astype(bf16)
        low = r.tmc[...].reshape(4, 2, 3, 2, 128).astype(bf16)
        for t in range(3):
            r.pa[t, :, pl.ds(2 * k, 2)] = hi[:, :, t]
            r.ca[t, :, pl.ds(2 * k, 2)] = low[:, :, t]
        return carry

    lax.fori_loop(0, 16, pack, 0)


def along_y_start(at, t, pairs, send, recv, own_sem):
    for n, (src, dst) in enumerate(pairs):
        for d, y, device in at.column():
            remote(src.at[t, y], dst.at[t, at.y], send.at[n, t], recv.at[n, t], device).start()
        pltpu.make_async_copy(src.at[t, at.y], dst.at[t, at.y], own_sem.at[n, t]).start()


def along_y_wait(at, t, pairs, send, recv, own_sem):
    for n, (src, dst) in enumerate(pairs):
        remote(src.at[t, pl.ds(0, 3)], dst.at[t, pl.ds(0, 3)], send.at[n, t], recv.at[n, t], 0).wait()
        pltpu.make_async_copy(src.at[t, at.y], dst.at[t, at.y], own_sem.at[n, t]).wait()


def to_grid_start(at, r, t):
    core, a = (0, t) if t < 2 else (1, 0)
    me = at.w * 2 + at.zl
    for n, (src, dst) in enumerate(((r.r1, r.xh), (r.c1, r.xc))):
        for chip, pc, p, zl, device in at.plane():
            if pc != core:
                continue
            piece, goal = src.at[t, :, p * 2 + zl], dst.at[a, me]
            copy = remote(piece, goal, r.s2.at[n, t], r.v2.at[n, a], device)
            if chip:
                pl.when(at.core != core)(lambda copy=copy: copy.start())
            else:
                copy.start()
        own = pltpu.make_async_copy(src.at[t, :, at.p * 2 + at.zl], dst.at[a, me], r.own_sem.at[n, a])
        pl.when(at.core == core)(lambda own=own: own.start())


def to_grid_arrived(at, r, a):
    me = at.w * 2 + at.zl
    for n, (src, dst) in enumerate(((r.r1, r.xh), (r.c1, r.xc))):
        some = dst.at[a, pl.ds(0, 63)]
        remote(some, some, r.s2.at[n, 0], r.v2.at[n, a], 0).wait_recv()
        pltpu.make_async_copy(src.at[0, :, 0], dst.at[a, me], r.own_sem.at[n, a]).wait()


def to_grid_sent(at, r, t):
    for n, src in enumerate((r.r1, r.c1)):
        for core in range(2):
            pieces = 31 if core == (0 if t < 2 else 1) else 32

            @pl.when(at.core == core)
            def _(n=n, src=src, pieces=pieces):
                some = src.at[t, :, pl.ds(0, pieces)]
                remote(some, some, r.s2.at[n, t], r.v2.at[n, 0], 0).wait_send()


def one_latitude(at, r, a):
    e = 3 * at.i + (a if a else jnp.where(at.core == 0, 0, 2))
    lane12 = lax.broadcasted_iota(jnp.int32, (2, 1, 128), 2)
    number = lax.broadcasted_iota(jnp.int32, (2, 1, 128), 0) * 12 + lane12
    weight = jnp.sum(jnp.where((number == e) & (lane12 < 12), r.lat[...], 0.0))
    for g in range(2):
        v = []
        for k in range(4):
            y, zl = 2 * g + k // 2, k % 2
            code = r.xc.reshape(2, 32, 2, 4, 2, 128)[a, :, zl, y].astype(f32).reshape(64, 128)
            first = jnp.floor(code * (1.0 / 16.0))
            r.steps[k, pl.ds(0, 64, stride=2), :] = first
            r.steps[k, pl.ds(1, 64, stride=2), :] = code - 16.0 * first
            v.append(decode(r.xh.reshape(2, 32, 2, 4, 4, 128)[a, :, zl, y].astype(f32).reshape(128, 128), r.steps[k]))
        for b, t in enumerate(block_transpose(v)):
            here = (slice(b * 128, (b + 1) * 128), slice(g * 128, (g + 1) * 128))
            r.xt[here], r.xl[here] = split(t)

    def inverse(rows, half):
        hi, lo, x, rest = r.ih[rows, half], r.il[rows, half], r.xt[half, :], r.xl[half, :]
        return nn(hi, x) + nn(lo, x) + nn(hi, rest)

    def columns(k, carry):
        rows = pl.ds(pl.multiple_of(k * 128, 128), 128)
        even, odd = inverse(rows, slice(0, 256)), inverse(rows, slice(256, 512))
        grid = jnp.concatenate([even + odd, even - odd], axis=0)
        v = grid.astype(bf16).astype(f32)
        scale = lax.rsqrt(jnp.mean(v * v, axis=1, keepdims=True) + EPS)
        n = (v * scale * r.gain_p[...]).astype(bf16)
        h = gelu(nt(n, r.w1p[...]) + r.b1[...]).astype(bf16)
        h = gelu(nt(h, r.w2v[...]) + r.b2[...]).astype(bf16)
        t = (nt(h, r.w3p[...]) + r.b3p[...]).astype(bf16)
        u = (grid + t.astype(f32)) * weight
        r.s_hi[rows, :], r.s_lo[rows, :] = split(u[:128] + u[128:])
        r.d_hi[rows, :], r.d_lo[rows, :] = split(u[:128] - u[128:])
        return carry

    lax.fori_loop(0, 3, columns, 0)

    def forward(half, hi, lo):
        return nn(r.fh[half, :], hi[...]) + nn(r.fh[half, :], lo[...]) + nn(r.fl[half, :], hi[...])

    even, odd = forward(slice(0, 256), r.s_hi, r.s_lo), forward(slice(256, 512), r.d_hi, r.d_lo)
    y = (even[:128], even[128:], odd[:128], odd[128:])
    for g in range(2):
        for k, t in enumerate(block_transpose([v[:, g * 128 : (g + 1) * 128] for v in y])):
            hi, step = encode(t)
            r.steps[k] = step
            code = 16.0 * r.steps[k, pl.ds(0, 64, stride=2), :] + r.steps[k, pl.ds(1, 64, stride=2), :]
            r.yh.reshape(2, 32, 2, 4, 4, 128)[a, :, k % 2, 2 * g + k // 2] = hi.reshape(32, 4, 128).astype(bf16)
            r.yc.reshape(2, 32, 2, 4, 2, 128)[a, :, k % 2, 2 * g + k // 2] = code.reshape(32, 2, 128).astype(bf16)


def network_weights(r):
    row = lax.broadcasted_iota(jnp.int32, (256, 256), 0)
    lane = lax.broadcasted_iota(jnp.int32, (256, 256), 1)
    pick = row == ((lane // 8) % 4) * 64 + (lane // 32) * 8 + lane % 8
    r.w1p[...] = nn(r.w1v[...], pick.astype(bf16)).astype(bf16)
    for k in range(8):
        for f in range(4):
            r.w3p[k * 32 + f * 8 : k * 32 + f * 8 + 8, :] = r.w3v[f * 64 + k * 8 : f * 64 + k * 8 + 8, :]
    for a, b in ((r.gain, r.gain_p), (r.b3, r.b3p)):
        rows = jnp.broadcast_to(a[...], (8, 256))
        b[...] = jnp.dot(rows, pick.astype(f32), precision=lax.Precision.HIGHEST, preferred_element_type=f32)[:1]


def send_latitude(at, r, a, mc):
    t = a if mc == 0 else 2
    me = at.p * 2 + at.zl
    for n, (src, dst) in enumerate(((r.yh, r.r2), (r.yc, r.c2))):
        for chip, core, p, zl, device in at.plane():
            if not (chip and core == mc):
                piece = src.at[a, (p * 2 + core) * 2 + zl]
                remote(piece, dst.at[t, :, me], r.s3.at[n, a], r.v3.at[n, t], device).start()
        pltpu.make_async_copy(src.at[a, at.w * 2 + at.zl], dst.at[t, :, me], r.own_sem.at[n, a]).start()


def latitude_own(at, r, a):
    for n, (src, dst) in enumerate(((r.yh, r.r2), (r.yc, r.c2))):
        pltpu.make_async_copy(src.at[a, 0], dst.at[0, :, 0], r.own_sem.at[n, a]).wait()


def latitude_sent(at, r, a):
    for n, src in enumerate((r.yh, r.yc)):
        some = src.at[a, pl.ds(0, 63)]
        remote(some, some, r.s3.at[n, a], r.v3.at[n, 0], 0).wait_send()


def wait_latitude(at, r, t):
    for n, dst in enumerate((r.r2, r.c2)):
        for core in range(2):
            pieces = 31 if core == (0 if t < 2 else 1) else 32

            @pl.when(at.core == core)
            def _(n=n, dst=dst, pieces=pieces):
                some = dst.at[t, :, pl.ds(0, pieces)]
                remote(some, some, r.s3.at[n, 0], r.v3.at[n, t], 0).wait_recv()


def legendre_back(at, r):
    def unpack(k, carry):
        hi = jnp.stack([r.vr[t, :, pl.ds(2 * k, 2)].astype(f32) for t in range(3)], axis=2)
        low = jnp.stack([r.vc[t, :, pl.ds(2 * k, 2)].astype(f32) for t in range(3)], axis=2)
        r.vs[pl.ds(pl.multiple_of(96 * k, 8), 96), :] = hi.reshape(96, 128)
        r.vcs[pl.ds(pl.multiple_of(48 * k, 8), 48), :] = low.reshape(48, 128)
        return carry

    lax.fori_loop(0, 16, unpack, 0)
    for q in range(4):
        code = r.vcs[pl.ds(q // 2, LAT, stride=2), :]
        first = jnp.floor(code * (1.0 / 16.0))
        step = first if q % 2 == 0 else code - 16.0 * first
        turned = decode(r.vs[pl.ds(q, LAT, stride=4), :], step).T
        for h in range(2):
            r.vt[2 * q + h], r.vl[2 * q + h] = split(turned[h * 64 : (h + 1) * 64])
    col = lax.broadcasted_iota(jnp.int32, (64, M), 1)
    field = (lax.broadcasted_iota(jnp.int32, (64, M), 0) // 8) % 4
    strength = jnp.where(
        field == 0, r.diff[0], jnp.where(field == 1, r.diff[1], jnp.where(field == 2, r.diff[2], r.diff[3]))
    )

    def damping(n, strength):
        g = (n * (n + 1)).astype(f32) / (M * (M - 1))
        return 1.0 + strength * (g * g)

    def level_rows(ref, i):
        return ref.at[:, pl.ds(pl.multiple_of(8 * i, 8), 8), :]

    def send_field_one(i):
        remote(r.f1.at[i], level_rows(r.g1, at.i), r.s5, r.v5, at.w * 8 + i).start()

    def wavenumber(k, carry):
        m = (at.i + 1 + k) % 8
        pl.when(k > 0)(lambda: send_field_one((at.i + k) % 8))
        n = 8 * at.w + m + col
        spec = nn(r.vt[m], r.leg_hi[m]) + nn(r.vt[m], r.leg_lo[m]) + nn(r.vl[m], r.leg_hi[m])
        spec = jnp.where(n < M, spec, 0.0)
        done = spec / damping(n, strength)
        for c in range(2):
            r.f1[m, c] = spec[c * 32 + 8 : c * 32 + 16]
            r.out[:, :, m, c, :] = done[c * 32 : (c + 1) * 32].reshape(F, 8, M)
        return carry

    with jax.named_scope("fall"):
        lax.fori_loop(0, 8, wavenumber, 0)
    own = pltpu.make_async_copy(r.f1.at[at.i], level_rows(r.g1, at.i), r.own_sem.at[0, 0])
    own.start()
    own.wait()
    n = 8 * at.w + at.i + col
    row = lax.broadcasted_iota(jnp.int32, (64, 64), 0)
    lane = lax.broadcasted_iota(jnp.int32, (64, 64), 1)
    rates = jnp.sum(jnp.where(row == lane, r.rates[...], 0.0), axis=1, keepdims=True)
    divisor = 1.0 + rates * (n * (n + 1)).astype(f32)
    damp = damping(n, r.diff[1])
    remote(r.f1.at[pl.ds(0, 7)], r.g1.at[:, pl.ds(0, 56), :], r.s5, r.v5, 0).wait_recv()
    for c in range(2):
        amplitude = lax.dot_general(
            r.modes[...], r.g1[c], (((0,), (0,)), ((), ())), precision=lax.Precision.HIGHEST, preferred_element_type=f32
        )
        solved = jnp.dot(
            r.modes[...], amplitude / divisor, precision=lax.Precision.HIGHEST, preferred_element_type=f32
        )
        r.hs[c] = solved / damp
    for d, i, device in at.level():
        remote(level_rows(r.hs, i), r.qs.at[at.i], r.s6, r.v6, device).start()
    own = pltpu.make_async_copy(level_rows(r.hs, at.i), r.qs.at[at.i], r.own_sem.at[1, 0])
    own.start()
    own.wait()
    remote(r.f1.at[pl.ds(0, 7)], r.g1.at[:, pl.ds(0, 56), :], r.s5, r.v5, 0).wait_send()
    remote(r.hs.at[:, pl.ds(0, 56), :], r.qs.at[pl.ds(0, 7)], r.s6, r.v6, 0).wait()
    for m in range(8):
        for c in range(2):
            r.out[1, :, m, c, :] = r.qs[m, c]


INPUTS = ["state_in", "leg", "lw", "modes", "rates", "diff", "gain", "w1", "b1", "w2", "b2", "w3", "b3", "ihh", "ilh", "fhh", "flh"]
DMA = pltpu.SemaphoreType.DMA
SCRATCH = dict(
    state=((F, 8, 8, 2, M), f32), leg_v=((8, LAT, M), f32), leg_hi=((8, LAT, M), bf16), leg_lo=((8, LAT, M), bf16), band=((4, LAT, 128), f32),
    tmp=((96, 128), f32), tmc=((48, 128), f32), pa=((3, 4, 32, 4, 128), bf16), ca=((3, 4, 32, 2, 128), bf16),
    r1=((3, 4, 32, 4, 128), bf16), c1=((3, 4, 32, 2, 128), bf16), xh=((2, 64, 4, 4, 128), bf16),
    xc=((2, 64, 4, 2, 128), bf16), lat=((2, 1, 128), f32), row=((1, 128), f32), w1v=((HID, 256), bf16),
    w2v=((HID, HID), bf16), w3v=((256, HID), bf16), ih=((HALF, 512), bf16), il=((HALF, 512), bf16),
    fh=((512, HALF), bf16), fl=((512, HALF), bf16), w1p=((HID, 256), bf16), w3p=((256, HID), bf16),
    gain_p=((1, 256), f32), b3p=((1, 256), f32), steps=((4, 128, 128), f32), xt=((512, 256), bf16),
    xl=((512, 256), bf16), s_hi=((HALF, 256), bf16), s_lo=((HALF, 256), bf16), d_hi=((HALF, 256), bf16),
    d_lo=((HALF, 256), bf16), yh=((2, 64, 4, 4, 128), bf16), yc=((2, 64, 4, 2, 128), bf16),
    r2=((3, 4, 32, 4, 128), bf16), c2=((3, 4, 32, 2, 128), bf16), vr=((3, 4, 32, 4, 128), bf16),
    vc=((3, 4, 32, 2, 128), bf16), vs=((1536, 128), f32), vcs=((768, 128), f32), vt=((8, 64, LAT), bf16),
    vl=((8, 64, LAT), bf16), f1=((8, 2, 8, M), f32), g1=((2, 64, M), f32), hs=((2, 64, M), f32),
    qs=((8, 2, 8, M), f32),
)
SEMS = dict(
    leg_sem=(8,), load_sem=(8,), own_sem=(2, 2), lat_sem=(3,), y_own=(2, 3), s1=(2, 3), v1=(2, 3), s2=(2, 3), v2=(2, 2),
    s3=(2, 2), v3=(2, 3), s4=(2, 3), v4=(2, 3), s5=(), v5=(), s6=(), v6=(),
)


class Refs:
    pass


def step_kernel(*refs):
    r = Refs()
    for name, ref in zip(INPUTS + ["out"] + list(SCRATCH) + list(SEMS), refs, strict=True):
        setattr(r, name, ref)
    at = Place()
    whole_state = pltpu.make_async_copy(r.state_in, r.state, r.load_sem.at[7])
    whole_state.start()
    pltpu.make_async_copy(r.leg.at[0], r.leg_v.at[0], r.leg_sem.at[0]).start()
    barrier, callers = meet(at)
    for m in range(1, 8):
        pltpu.make_async_copy(r.leg.at[m], r.leg_v.at[m], r.leg_sem.at[m]).start()
    loads = [
        pltpu.make_async_copy(a, b, r.load_sem.at[n])
        for n, (a, b) in enumerate(
            ((r.w1, r.w1v), (r.w3, r.w3v), (r.w2, r.w2v), (r.ihh, r.ih), (r.ilh, r.il), (r.fhh, r.fh), (r.flh, r.fl))
        )
    ]
    for load in loads:
        load.start()
    lane = lax.broadcasted_iota(jnp.int32, (1, 128), 1)
    row = jnp.zeros((1, 128), f32)
    for k in range(12):
        row = jnp.where(lane == k, r.lw[k], row)
    r.row[...] = row
    whole_state.wait()
    with jax.named_scope('legfwd'):
        legendre_forward(at, r)
    with jax.named_scope('barwait'):
        pl.semaphore_wait(barrier, callers)
    weights = remote(r.row, r.lat.at[at.core], r.lat_sem.at[0], r.lat_sem.at[1], (at.w + 1 - 2 * at.core) * 8 + at.i)
    weights.start()
    own = pltpu.make_async_copy(r.row, r.lat.at[at.core], r.lat_sem.at[2])
    own.start()
    sc = jax.named_scope
    order = (0, 2, 1)
    there = (((r.pa, r.r1), (r.ca, r.c1)), r.s1, r.v1, r.y_own)
    back = (((r.r2, r.vr), (r.c2, r.vc)), r.s4, r.v4, r.y_own)
    with sc("y1"):
        for t in order:
            along_y_start(at, t, *there)
        for t in order:
            along_y_wait(at, t, *there)
            to_grid_start(at, r, t)
    with sc("weights"):
        own.wait()
        weights.wait()
        for load in loads:
            load.wait()
        network_weights(r)
    with sc("arrive0"):
        to_grid_arrived(at, r, 0)
    with sc("lat0"):
        one_latitude(at, r, 0)

    @pl.when(at.core == 0)
    def _():
        with sc("send0"):
            send_latitude(at, r, 0, 0)
        with sc("arrive1"):
            to_grid_arrived(at, r, 1)
        with sc("lat1"):
            one_latitude(at, r, 1)
        with sc("send1"):
            send_latitude(at, r, 1, 0)
            latitude_own(at, r, 0)
            latitude_own(at, r, 1)

    @pl.when(at.core == 1)
    def _():
        with sc("send"):
            send_latitude(at, r, 0, 1)
            latitude_own(at, r, 0)

    with sc("y2"):
        for t in order:
            wait_latitude(at, r, t)
            along_y_start(at, t, *back)
        for t in order:
            along_y_wait(at, t, *back)
    with sc("legback"):
        legendre_back(at, r)
    with sc("sent"):
        for t in order:
            to_grid_sent(at, r, t)
        latitude_sent(at, r, 0)
        pl.when(at.core == 0)(lambda: latitude_sent(at, r, 1))


VMEM = pl.BlockSpec(memory_space=pltpu.VMEM)
SMEM = pl.BlockSpec(memory_space=pltpu.SMEM)
ANY = pl.BlockSpec(memory_space=pl.ANY)


def body(state, legendre, lat_weight, modes, mode_rates, diffusion, norm_gain, w_first, b_first, w_second, b_second, w_third, b_third):
    return pl.pallas_call(
        step_kernel,
        name="step",
        out_shape=pltpu.VMEM((F, 8, 8, 2, M), f32),
        in_specs=[ANY, ANY, SMEM, VMEM, VMEM, SMEM, VMEM, ANY, VMEM, ANY, VMEM, ANY, VMEM, ANY, ANY, ANY, ANY],
        out_specs=VMEM,
        scratch_shapes=[pltpu.VMEM(*s) for s in SCRATCH.values()] + [DMA(s) if s else DMA for s in SEMS.values()],
        compiler_params=pltpu.CompilerParams(collective_id=0, has_side_effects=True),
    )(
        state, legendre, lat_weight, modes, mode_rates.reshape(1, LEV), diffusion, norm_gain.reshape(1, 256), w_first,
        b_first.reshape(1, HID), w_second, b_second.reshape(1, HID), w_third, b_third.reshape(1, 256),
        *[jnp.asarray(t) for t in tables()],
    )


def solution(mesh):
    return jax.shard_map(
        body,
        mesh=mesh,
        in_specs=(P(None, "level", "wave", None, None), P("wave", None, None), P("wave")) + (P(),) * 10,
        out_specs=P(None, "level", "wave", None, None),
        check_vma=False,
    )
```

```python
import jax
import jax.numpy as jnp
import numpy as np
from jax import lax
from jax.experimental import pallas as pl
from jax.experimental.pallas import tpu as pltpu
from jax.sharding import PartitionSpec as P

F, LEV, M, LAT, LON, HID = 4, 64, 256, 384, 768, 1024
HALF = LON // 2
EPS = 1e-06
LOGICAL = pl.DeviceIdType.LOGICAL
bf16, f32 = jnp.bfloat16, jnp.float32


def tables():
    b = np.arange(4)[:, None]
    r = np.arange(128)[None, :]
    m = (8 * (r // 4) + 2 * (r % 4) + b // 2).reshape(-1)
    c = np.broadcast_to(b % 2, (4, 128)).reshape(-1)
    o = np.arange(HALF)
    angle = 2.0 * np.pi * ((m[:, None] * o[None, :]) % LON) / LON
    wave = np.where(c[:, None] == 0, np.cos(angle), -np.sin(angle))
    inverse = (np.where(m == 0, 1.0, 2.0)[:, None] * wave).T.astype(np.float32)
    forward = (wave / LON).astype(np.float32)
    parts = []
    for t in (inverse, forward):
        hi = t.astype(jnp.bfloat16)
        parts += [hi, (t - hi.astype(np.float32)).astype(jnp.bfloat16)]
    return parts


def split(x):
    hi = x.astype(bf16)
    return hi, (x - hi.astype(f32)).astype(bf16)


def encode(x, steps):
    hi = x.astype(bf16).astype(f32)
    size = jnp.abs(hi)
    r = jnp.where(size > 0.0, (x - hi) / size, 0.0)
    return hi, jnp.clip(jnp.floor(r * (128.0 * steps) + 0.5 * steps), 0.0, steps - 1.0)


def decode(hi, k, steps):
    return hi + jnp.abs(hi) * ((k - (0.5 * steps - 0.5)) * (1.0 / (128.0 * steps)))


def gelu(x):
    c = 0.7978845608028654
    half = 0.5 * x
    return half + half * jnp.tanh(x * (c + (c * 0.044715) * (x * x)))


def nn(a, b):
    return lax.dot_general(a, b, (((1,), (0,)), ((), ())), preferred_element_type=f32)


def nt(a, b):
    return lax.dot_general(a, b, (((1,), (1,)), ((), ())), preferred_element_type=f32)


def block_transpose(v):
    lane = lax.broadcasted_iota(jnp.int32, v[0].shape, 1)
    low, even = lane < 64, (lane % 64) < 32
    l02 = jnp.where(low, v[0], pltpu.roll(v[2], 64, 1))
    h02 = jnp.where(low, pltpu.roll(v[0], 64, 1), v[2])
    l13 = jnp.where(low, v[1], pltpu.roll(v[3], 64, 1))
    h13 = jnp.where(low, pltpu.roll(v[1], 64, 1), v[3])
    return [
        jnp.where(even, l02, pltpu.roll(l13, 32, 1)),
        jnp.where(even, pltpu.roll(l02, 96, 1), l13),
        jnp.where(even, h02, pltpu.roll(h13, 32, 1)),
        jnp.where(even, pltpu.roll(h02, 96, 1), h13),
    ]


class Place:
    def __init__(self):
        self.w, self.i = lax.axis_index("wave"), lax.axis_index("level")
        w, i = self.w, self.i
        self.p, self.core, self.y, self.zl = w // 2, w % 2, i // 2, i % 2
        x, z = w // 8, ((w // 2) % 4) * 2 + i % 2
        self.xs = [(x + d) % 4 for d in range(4)]
        self.zs = [(z + d) % 8 for d in range(8)]
        self.ys = [(self.y + d) % 4 for d in range(4)]

    def plane(self):
        for dz in (4, 3, 5, 2, 6, 1, 7, 0):
            for dx in (2, 1, 3, 0):
                zh, zl = self.zs[dz] // 2, self.zs[dz] % 2
                p = self.xs[dx] * 4 + zh
                for core in (0, 1):
                    yield dz == 0 and dx == 0, core, p, zl, p * 16 + core * 8 + self.y * 2 + zl

    def level(self):
        for d in (4, 2, 6, 3, 5, 1, 7):
            i = (self.i + d) % 8
            yield d, i, self.w * 8 + i

    def column(self):
        for d in (2, 1, 3):
            yield d, self.ys[d], self.w * 8 + self.ys[d] * 2 + self.zl


def remote(src, dst, send, recv, device):
    return pltpu.make_async_remote_copy(src, dst, send, recv, device_id=device, device_id_type=LOGICAL)


def meet(at):
    barrier = pltpu.get_barrier_semaphore()
    for d, i, device in at.level():
        pl.semaphore_signal(barrier, inc=1, device_id=device, device_id_type=LOGICAL)
    buddy = (at.w + 1 - 2 * at.core) * 8 + at.i
    pl.semaphore_signal(barrier, inc=1, device_id=buddy, device_id_type=LOGICAL)
    for dz in (4, 3, 5, 2, 6, 1, 7, 0):
        for dx in (2, 1, 3, 0):
            if dz == 0 and dx == 0:
                continue
            zh, zl = at.zs[dz] // 2, at.zs[dz] % 2
            for core in (0, 1):
                device = ((at.xs[dx] * 4 + zh) * 2 + core) * 8 + at.y * 2 + zl
                pl.semaphore_signal(barrier, inc=1, device_id=device, device_id_type=LOGICAL)
    return barrier, 7 + 1 + 62 + 0


def legendre_forward(at, r):
    w = at.w
    col = lax.broadcasted_iota(jnp.int32, (64, M), 1)

    def pair(q, carry):
        acc = jnp.zeros((LAT, 128), f32)
        for h in range(2):
            m = 2 * q + h
            s = jnp.concatenate([r.state[:, :, m, c, :].reshape(32, M) for c in range(2)], axis=0)
            s = jnp.where(col < M - (8 * w + m), s, 0.0)
            hi, lo = split(s)
            zero = jnp.zeros_like(hi)
            order = (hi, zero, lo, zero) if h == 0 else (zero, hi, zero, lo)
            right = jnp.concatenate(order, axis=0)
            pltpu.make_async_copy(r.leg.at[m], r.leg_v.at[m], r.leg_sem.at[m]).wait()
            bhi, blo = split(r.leg_v[m])
            r.leg_hi[m] = bhi
            r.leg_lo[m] = blo
            both = nt(bhi, right)
            acc += both[:, :128] + both[:, 128:] + nt(blo, right[:128])
        r.band[q] = acc
        return carry

    lax.fori_loop(0, 4, pair, 0)

    def pack(k, carry):
        code = []
        for q in range(4):
            hi, step = encode(r.band[q, pl.ds(pl.multiple_of(24 * k, 8), 24), :], 16)
            r.tmp[pl.ds(q, 24, stride=4), :] = hi
            code.append(step)
        r.tmc[pl.ds(0, 24, stride=2), :] = 16.0 * code[0] + code[1]
        r.tmc[pl.ds(1, 24, stride=2), :] = 16.0 * code[2] + code[3]
        hi = r.tmp[...].reshape(4, 2, 3, 4, 128).astype(bf16)
        low = r.tmc[...].reshape(4, 2, 3, 2, 128).astype(bf16)
        for t in range(3):
            r.pa[t, :, pl.ds(2 * k, 2)] = hi[:, :, t]
            r.ca[t, :, pl.ds(2 * k, 2)] = low[:, :, t]
        return carry

    lax.fori_loop(0, 16, pack, 0)


def third(src, t, y):
    return src.at[t, y] if src.shape[1] == 4 else src.at[t, y // 2]


def along_y_start(at, t, pairs, send, recv, own_sem):
    for n, (src, dst) in enumerate(pairs):
        for d, y, device in at.column():
            remote(third(src, t, y), dst.at[t, at.y], send.at[n, t], recv.at[n, t], device).start()
        pltpu.make_async_copy(third(src, t, at.y), dst.at[t, at.y], own_sem.at[n, t]).start()


def along_y_wait(at, t, pairs, send, recv, own_sem):
    for n, (src, dst) in enumerate(pairs):
        some = dst.at[t, pl.ds(0, 3)]
        remote(some, some, send.at[n, t], recv.at[n, t], 0).wait()
        pltpu.make_async_copy(third(src, t, at.y), dst.at[t, at.y], own_sem.at[n, t]).wait()


def to_grid_start(at, r, t):
    core, a = (0, t) if t < 2 else (1, 0)
    me = at.w * 2 + at.zl
    for n, (src, dst) in enumerate(((r.r1, r.xh), (r.c1, r.xc))):
        for chip, pc, p, zl, device in at.plane():
            if pc != core:
                continue
            piece, goal = src.at[t, :, p * 2 + zl], dst.at[a, me]
            copy = remote(piece, goal, r.s2.at[n, t], r.v2.at[n, a], device)
            if chip:
                pl.when(at.core != core)(lambda copy=copy: copy.start())
            else:
                copy.start()
        own = pltpu.make_async_copy(src.at[t, :, at.p * 2 + at.zl], dst.at[a, me], r.own_sem.at[n, a])
        pl.when(at.core == core)(lambda own=own: own.start())


def to_grid_arrived(at, r, a):
    me = at.w * 2 + at.zl
    for n, (src, dst) in enumerate(((r.r1, r.xh), (r.c1, r.xc))):
        some = dst.at[a, pl.ds(0, 63)]
        remote(some, some, r.s2.at[n, 0], r.v2.at[n, a], 0).wait_recv()
        pltpu.make_async_copy(src.at[0, :, 0], dst.at[a, me], r.own_sem.at[n, a]).wait()


def to_grid_sent(at, r, t):
    for n, src in enumerate((r.r1, r.c1)):
        for core in range(2):
            pieces = 31 if core == (0 if t < 2 else 1) else 32

            @pl.when(at.core == core)
            def _(n=n, src=src, pieces=pieces):
                some = src.at[t, :, pl.ds(0, pieces)]
                remote(some, some, r.s2.at[n, t], r.v2.at[n, 0], 0).wait_send()


def one_latitude(at, r, a):
    e = 3 * at.i + (a if a else jnp.where(at.core == 0, 0, 2))
    lane12 = lax.broadcasted_iota(jnp.int32, (2, 1, 128), 2)
    number = lax.broadcasted_iota(jnp.int32, (2, 1, 128), 0) * 12 + lane12
    weight = jnp.sum(jnp.where((number == e) & (lane12 < 12), r.lat[...], 0.0))
    for g in range(2):
        v = []
        for k in range(4):
            y, zl = 2 * g + k // 2, k % 2
            code = r.xc.reshape(2, 32, 2, 4, 2, 128)[a, :, zl, y].astype(f32).reshape(64, 128)
            first = jnp.floor(code * (1.0 / 16.0))
            r.steps[k, pl.ds(0, 64, stride=2), :] = first
            r.steps[k, pl.ds(1, 64, stride=2), :] = code - 16.0 * first
            v.append(decode(r.xh.reshape(2, 32, 2, 4, 4, 128)[a, :, zl, y].astype(f32).reshape(128, 128), r.steps[k], 16))
        for b, t in enumerate(block_transpose(v)):
            here = (slice(b * 128, (b + 1) * 128), slice(g * 128, (g + 1) * 128))
            r.xt[here], r.xl[here] = split(t)

    def inverse(rows, half):
        hi, lo, x, rest = r.ih[rows, half], r.il[rows, half], r.xt[half, :], r.xl[half, :]
        return nn(hi, x) + nn(lo, x) + nn(hi, rest)

    def columns(k, carry):
        rows = pl.ds(pl.multiple_of(k * 192, 64), 192)
        even, odd = inverse(rows, slice(0, 256)), inverse(rows, slice(256, 512))
        grid = jnp.concatenate([even + odd, even - odd], axis=0)
        v = grid.astype(bf16).astype(f32)
        scale = lax.rsqrt(jnp.mean(v * v, axis=1, keepdims=True) + EPS)
        n = (v * scale * r.gain_p[...]).astype(bf16)
        h = gelu(nt(n, r.w1p[...]) + r.b1[...]).astype(bf16)
        h = gelu(nt(h, r.w2v[...]) + r.b2[...]).astype(bf16)
        t = (nt(h, r.w3p[...]) + r.b3p[...]).astype(bf16)
        u = (grid + t.astype(f32)) * weight
        r.s_hi[rows, :], r.s_lo[rows, :] = split(u[:192] + u[192:])
        r.d_hi[rows, :], r.d_lo[rows, :] = split(u[:192] - u[192:])
        return carry

    lax.fori_loop(0, 2, columns, 0)

    def forward(half, hi, lo):
        return nn(r.fh[half, :], hi[...]) + nn(r.fh[half, :], lo[...]) + nn(r.fl[half, :], hi[...])

    even, odd = forward(slice(0, 256), r.s_hi, r.s_lo), forward(slice(256, 512), r.d_hi, r.d_lo)
    y = (even[:128], even[128:], odd[:128], odd[128:])
    for g in range(2):
        code = []
        for k, t in enumerate(block_transpose([v[:, g * 128 : (g + 1) * 128] for v in y])):
            hi, step = encode(t, 4)
            r.steps[k] = step
            rows = [r.steps[k, pl.ds(q, 32, stride=4), :] for q in range(4)]
            code.append(64.0 * rows[0] + 16.0 * rows[1] + (4.0 * rows[2] + rows[3]))
            r.yh.reshape(2, 32, 2, 4, 4, 128)[a, :, k % 2, 2 * g + k // 2] = hi.reshape(32, 4, 128).astype(bf16)
        for zl in range(2):
            both = jnp.stack([code[zl], code[zl + 2]], axis=1)
            r.yc.reshape(2, 32, 2, 2, 2, 128)[a, :, zl, g] = both.astype(bf16)


def network_weights(r):
    row = lax.broadcasted_iota(jnp.int32, (256, 256), 0)
    lane = lax.broadcasted_iota(jnp.int32, (256, 256), 1)
    pick = row == ((lane // 8) % 4) * 64 + (lane // 32) * 8 + lane % 8
    r.w1p[...] = nn(r.w1v[...], pick.astype(bf16)).astype(bf16)
    for k in range(8):
        for f in range(4):
            r.w3p[k * 32 + f * 8 : k * 32 + f * 8 + 8, :] = r.w3v[f * 64 + k * 8 : f * 64 + k * 8 + 8, :]
    for a, b in ((r.gain, r.gain_p), (r.b3, r.b3p)):
        rows = jnp.broadcast_to(a[...], (8, 256))
        b[...] = jnp.dot(rows, pick.astype(f32), precision=lax.Precision.HIGHEST, preferred_element_type=f32)[:1]


def send_latitude(at, r, a, mc):
    t = a if mc == 0 else 2
    me = at.p * 2 + at.zl
    for n, (src, dst) in enumerate(((r.yh, r.r2), (r.yc, r.c2))):
        for chip, core, p, zl, device in at.plane():
            if not (chip and core == mc):
                piece = src.at[a, (p * 2 + core) * 2 + zl]
                remote(piece, dst.at[t, :, me], r.s3.at[n, a], r.v3.at[n, t], device).start()
        pltpu.make_async_copy(src.at[a, at.w * 2 + at.zl], dst.at[t, :, me], r.own_sem.at[n, a]).start()


def latitude_own(at, r, a):
    for n, (src, dst) in enumerate(((r.yh, r.r2), (r.yc, r.c2))):
        pltpu.make_async_copy(src.at[a, 0], dst.at[0, :, 0], r.own_sem.at[n, a]).wait()


def latitude_sent(at, r, a):
    for n, src in enumerate((r.yh, r.yc)):
        some = src.at[a, pl.ds(0, 63)]
        remote(some, some, r.s3.at[n, a], r.v3.at[n, 0], 0).wait_send()


def wait_latitude(at, r, t):
    for n, dst in enumerate((r.r2, r.c2)):
        for core in range(2):
            pieces = 31 if core == (0 if t < 2 else 1) else 32

            @pl.when(at.core == core)
            def _(n=n, dst=dst, pieces=pieces):
                some = dst.at[t, :, pl.ds(0, pieces)]
                remote(some, some, r.s3.at[n, 0], r.v3.at[n, t], 0).wait_recv()


def legendre_back(at, r):
    def unpack(k, carry):
        hi = jnp.stack([r.vr[t, :, pl.ds(2 * k, 2)].astype(f32) for t in range(3)], axis=2)
        tiles = [r.vc[t, :, pl.ds(2 * k, 2)].astype(f32) for t in range(3)]
        low = jnp.stack([jnp.where(at.y % 2 == 0, v[:, :, 0], v[:, :, 1]) for v in tiles], axis=2)
        r.vs[pl.ds(pl.multiple_of(96 * k, 8), 96), :] = hi.reshape(96, 128)
        r.vcs[pl.ds(pl.multiple_of(24 * k, 8), 24), :] = low.reshape(24, 128)
        return carry

    lax.fori_loop(0, 16, unpack, 0)
    rest = r.vcs[...]
    for q, unit in enumerate((64.0, 16.0, 4.0, 1.0)):
        step = jnp.floor(rest * (1.0 / unit))
        rest = rest - unit * step
        turned = decode(r.vs[pl.ds(q, LAT, stride=4), :], step, 4).T
        for h in range(2):
            r.vt[2 * q + h], r.vl[2 * q + h] = split(turned[h * 64 : (h + 1) * 64])
    col = lax.broadcasted_iota(jnp.int32, (64, M), 1)
    field = (lax.broadcasted_iota(jnp.int32, (64, M), 0) // 8) % 4
    strength = jnp.where(
        field == 0, r.diff[0], jnp.where(field == 1, r.diff[1], jnp.where(field == 2, r.diff[2], r.diff[3]))
    )

    def damping(n, strength):
        g = (n * (n + 1)).astype(f32) / (M * (M - 1))
        return 1.0 + strength * (g * g)

    def level_rows(ref, i):
        return ref.at[:, pl.ds(pl.multiple_of(8 * i, 8), 8), :]

    def send_field_one(i):
        remote(r.f1.at[i], level_rows(r.g1, at.i), r.s5, r.v5, at.w * 8 + i).start()

    def wavenumber(k, carry):
        m = (at.i + 1 + k) % 8
        pl.when(k > 0)(lambda: send_field_one((at.i + k) % 8))
        n = 8 * at.w + m + col
        spec = nn(r.vt[m], r.leg_hi[m]) + nn(r.vt[m], r.leg_lo[m]) + nn(r.vl[m], r.leg_hi[m])
        spec = jnp.where(n < M, spec, 0.0)
        done = spec / damping(n, strength)
        for c in range(2):
            r.f1[m, c] = spec[c * 32 + 8 : c * 32 + 16]
            r.out[:, :, m, c, :] = done[c * 32 : (c + 1) * 32].reshape(F, 8, M)
        return carry

    with jax.named_scope("fall"):
        lax.fori_loop(0, 8, wavenumber, 0)
    own = pltpu.make_async_copy(r.f1.at[at.i], level_rows(r.g1, at.i), r.own_sem.at[0, 0])
    own.start()
    own.wait()
    n = 8 * at.w + at.i + col
    row = lax.broadcasted_iota(jnp.int32, (64, 64), 0)
    lane = lax.broadcasted_iota(jnp.int32, (64, 64), 1)
    rates = jnp.sum(jnp.where(row == lane, r.rates[...], 0.0), axis=1, keepdims=True)
    divisor = 1.0 + rates * (n * (n + 1)).astype(f32)
    damp = damping(n, r.diff[1])
    remote(r.f1.at[pl.ds(0, 7)], r.g1.at[:, pl.ds(0, 56), :], r.s5, r.v5, 0).wait_recv()
    for c in range(2):
        amplitude = lax.dot_general(
            r.modes[...], r.g1[c], (((0,), (0,)), ((), ())), precision=lax.Precision.HIGHEST, preferred_element_type=f32
        )
        solved = jnp.dot(
            r.modes[...], amplitude / divisor, precision=lax.Precision.HIGHEST, preferred_element_type=f32
        )
        r.hs[c] = solved / damp
    for d, i, device in at.level():
        remote(level_rows(r.hs, i), r.qs.at[at.i], r.s6, r.v6, device).start()
    own = pltpu.make_async_copy(level_rows(r.hs, at.i), r.qs.at[at.i], r.own_sem.at[1, 0])
    own.start()
    own.wait()
    remote(r.f1.at[pl.ds(0, 7)], r.g1.at[:, pl.ds(0, 56), :], r.s5, r.v5, 0).wait_send()
    remote(r.hs.at[:, pl.ds(0, 56), :], r.qs.at[pl.ds(0, 7)], r.s6, r.v6, 0).wait()
    for m in range(8):
        for c in range(2):
            r.out[1, :, m, c, :] = r.qs[m, c]


INPUTS = ["state_in", "leg", "lw", "modes", "rates", "diff", "gain", "w1", "b1", "w2", "b2", "w3", "b3", "ihh", "ilh", "fhh", "flh"]
DMA = pltpu.SemaphoreType.DMA
SCRATCH = dict(
    state=((F, 8, 8, 2, M), f32), leg_v=((8, LAT, M), f32), leg_hi=((8, LAT, M), bf16), leg_lo=((8, LAT, M), bf16), band=((4, LAT, 128), f32),
    tmp=((96, 128), f32), tmc=((48, 128), f32), pa=((3, 4, 32, 4, 128), bf16), ca=((3, 4, 32, 2, 128), bf16),
    r1=((3, 4, 32, 4, 128), bf16), c1=((3, 4, 32, 2, 128), bf16), xh=((2, 64, 4, 4, 128), bf16),
    xc=((2, 64, 4, 2, 128), bf16), lat=((2, 1, 128), f32), row=((1, 128), f32), w1v=((HID, 256), bf16),
    w2v=((HID, HID), bf16), w3v=((256, HID), bf16), ih=((HALF, 512), bf16), il=((HALF, 512), bf16),
    fh=((512, HALF), bf16), fl=((512, HALF), bf16), w1p=((HID, 256), bf16), w3p=((256, HID), bf16),
    gain_p=((1, 256), f32), b3p=((1, 256), f32), steps=((4, 128, 128), f32), xt=((512, 256), bf16),
    xl=((512, 256), bf16), s_hi=((HALF, 256), bf16), s_lo=((HALF, 256), bf16), d_hi=((HALF, 256), bf16),
    d_lo=((HALF, 256), bf16), yh=((2, 64, 4, 4, 128), bf16), yc=((2, 64, 2, 2, 128), bf16),
    r2=((3, 4, 32, 4, 128), bf16), c2=((3, 2, 32, 2, 128), bf16), vr=((3, 4, 32, 4, 128), bf16),
    vc=((3, 4, 32, 2, 128), bf16), vs=((1536, 128), f32), vcs=((LAT, 128), f32), vt=((8, 64, LAT), bf16),
    vl=((8, 64, LAT), bf16), f1=((8, 2, 8, M), f32), g1=((2, 64, M), f32), hs=((2, 64, M), f32),
    qs=((8, 2, 8, M), f32),
)
SEMS = dict(
    leg_sem=(8,), load_sem=(8,), own_sem=(2, 2), lat_sem=(3,), y_own=(2, 3), s1=(2, 3), v1=(2, 3), s2=(2, 3), v2=(2, 2),
    s3=(2, 2), v3=(2, 3), s4=(2, 3), v4=(2, 3), s5=(), v5=(), s6=(), v6=(),
)


class Refs:
    pass


def step_kernel(*refs):
    r = Refs()
    for name, ref in zip(INPUTS + ["out"] + list(SCRATCH) + list(SEMS), refs, strict=True):
        setattr(r, name, ref)
    at = Place()
    whole_state = pltpu.make_async_copy(r.state_in, r.state, r.load_sem.at[7])
    whole_state.start()
    pltpu.make_async_copy(r.leg.at[0], r.leg_v.at[0], r.leg_sem.at[0]).start()
    barrier, callers = meet(at)
    for m in range(1, 8):
        pltpu.make_async_copy(r.leg.at[m], r.leg_v.at[m], r.leg_sem.at[m]).start()
    loads = [
        pltpu.make_async_copy(a, b, r.load_sem.at[n])
        for n, (a, b) in enumerate(
            ((r.w1, r.w1v), (r.w3, r.w3v), (r.w2, r.w2v), (r.ihh, r.ih), (r.ilh, r.il), (r.fhh, r.fh), (r.flh, r.fl))
        )
    ]
    for load in loads:
        load.start()
    lane = lax.broadcasted_iota(jnp.int32, (1, 128), 1)
    row = jnp.zeros((1, 128), f32)
    for k in range(12):
        row = jnp.where(lane == k, r.lw[k], row)
    r.row[...] = row
    whole_state.wait()
    with jax.named_scope('legfwd'):
        legendre_forward(at, r)
    with jax.named_scope('barwait'):
        pl.semaphore_wait(barrier, callers)
    weights = remote(r.row, r.lat.at[at.core], r.lat_sem.at[0], r.lat_sem.at[1], (at.w + 1 - 2 * at.core) * 8 + at.i)
    weights.start()
    own = pltpu.make_async_copy(r.row, r.lat.at[at.core], r.lat_sem.at[2])
    own.start()
    sc = jax.named_scope
    order = (0, 2, 1)
    there = (((r.pa, r.r1), (r.ca, r.c1)), r.s1, r.v1, r.y_own)
    back = (((r.r2, r.vr), (r.c2, r.vc)), r.s4, r.v4, r.y_own)
    with sc("y1"):
        for t in order:
            along_y_start(at, t, *there)
        for t in order:
            along_y_wait(at, t, *there)
            to_grid_start(at, r, t)
    with sc("weights"):
        own.wait()
        weights.wait()
        for load in loads:
            load.wait()
        network_weights(r)
    with sc("arrive0"):
        to_grid_arrived(at, r, 0)
    with sc("lat0"):
        one_latitude(at, r, 0)

    @pl.when(at.core == 0)
    def _():
        with sc("send0"):
            send_latitude(at, r, 0, 0)
        with sc("arrive1"):
            to_grid_arrived(at, r, 1)
        with sc("lat1"):
            one_latitude(at, r, 1)
        with sc("send1"):
            send_latitude(at, r, 1, 0)
            latitude_own(at, r, 0)
            latitude_own(at, r, 1)

    @pl.when(at.core == 1)
    def _():
        with sc("send"):
            send_latitude(at, r, 0, 1)
            latitude_own(at, r, 0)

    with sc("y2"):
        for t in order:
            wait_latitude(at, r, t)
            along_y_start(at, t, *back)
        for t in order:
            along_y_wait(at, t, *back)
    with sc("legback"):
        legendre_back(at, r)
    with sc("sent"):
        for t in order:
            to_grid_sent(at, r, t)
        latitude_sent(at, r, 0)
        pl.when(at.core == 0)(lambda: latitude_sent(at, r, 1))


VMEM = pl.BlockSpec(memory_space=pltpu.VMEM)
SMEM = pl.BlockSpec(memory_space=pltpu.SMEM)
ANY = pl.BlockSpec(memory_space=pl.ANY)


def body(state, legendre, lat_weight, modes, mode_rates, diffusion, norm_gain, w_first, b_first, w_second, b_second, w_third, b_third):
    return pl.pallas_call(
        step_kernel,
        name="step",
        out_shape=pltpu.VMEM((F, 8, 8, 2, M), f32),
        in_specs=[ANY, ANY, SMEM, VMEM, VMEM, SMEM, VMEM, ANY, VMEM, ANY, VMEM, ANY, VMEM, ANY, ANY, ANY, ANY],
        out_specs=VMEM,
        scratch_shapes=[pltpu.VMEM(*s) for s in SCRATCH.values()] + [DMA(s) if s else DMA for s in SEMS.values()],
        compiler_params=pltpu.CompilerParams(collective_id=0, has_side_effects=True),
    )(
        state, legendre, lat_weight, modes, mode_rates.reshape(1, LEV), diffusion, norm_gain.reshape(1, 256), w_first,
        b_first.reshape(1, HID), w_second, b_second.reshape(1, HID), w_third, b_third.reshape(1, 256),
        *[jnp.asarray(t) for t in tables()],
    )


def solution(mesh):
    return jax.shard_map(
        body,
        mesh=mesh,
        in_specs=(P(None, "level", "wave", None, None), P("wave", None, None), P("wave")) + (P(),) * 10,
        out_specs=P(None, "level", "wave", None, None),
        check_vma=False,
    )
```
